256 devices in a mesh: frame: 32 (over z, y_lo, core), rec: 8 (over y_hi, x).
Axes of the slice: x: 4, y: 4 (y_hi: 2, y_lo: 2; y = y_hi * 2 + y_lo), z: 8, core: 2. Of those that a mesh axis runs over, the one named last changes fastest.
Arguments:
- code_indices: int32 [8, 8192, 8], P('rec', 'frame'), may hold values from 0 to 7
- lengths: int32 [8], P('rec'), may hold values from 4096 to 8192
- cotangent: bfloat16 [8, 2621440], P('rec', 'frame'), may hold values from -6 to 6
- embed_weight: float32 [8, 512], replicated, may hold values from -2 to 2
- embed_bias: float32 [512], replicated, may hold values from -3 to 3
- depth_kernel: float32 [7, 512], replicated, may hold values from -2 to 2
- depth_bias: float32 [512], replicated, may hold values from -3 to 3
- norm_gain: float32 [512], replicated, may hold values from 0.5 to 1.5
- norm_bias: float32 [512], replicated, may hold values from -1.75 to 1.75
- up_weight: bfloat16 [512, 1536], replicated, may hold values from -0.25 to 0.25
- up_bias: float32 [1536], replicated, may hold values from -3 to 3
- down_weight: bfloat16 [1536, 512], replicated, may hold values from -0.15625 to 0.15625
- down_bias: float32 [512], replicated, may hold values from -1.75 to 1.75
- layer_scale: float32 [512], replicated, may hold values from 0.3 to 1
- head_weight: bfloat16 [512, 1280], replicated, may hold values from -0.25 to 0.25
- head_bias: float32 [1280], replicated, may hold values from -3 to 3
Outputs:
- embed_weight_grad: float32 [8, 512], P(None, 'frame')
- embed_bias_grad: float32 [512], P('frame')
- depth_kernel_grad: float32 [7, 512], P(None, 'frame')
- depth_bias_grad: float32 [512], P('frame')
- norm_gain_grad: float32 [512], P('frame')
- norm_bias_grad: float32 [512], P('frame')
- up_weight_grad: float32 [512, 1536], P('frame')
- up_bias_grad: float32 [1536], P('frame')
- down_weight_grad: float32 [1536, 512], P('frame')
- down_bias_grad: float32 [512], P('frame')
- layer_scale_grad: float32 [512], P('frame')
- head_weight_grad: float32 [512, 1280], P('frame')
- head_bias_grad: float32 [1280], P('frame')
The draws below stay inside these ranges and needn't reach their ends.
Inputs may be any that keep to these rules, and one draw needn't show every extreme that they name: `lengths`: frames at or after a recording's length are padding.
All inputs are finite; a program needn't handle non-finite values.
Results may differ from the reference program's by a relative error of at most 0.011.
Values may be sent and summed in bfloat16 or wider, within the bound.
No kernel may reach another device: no remote copies, remote signals or barrier semaphores. Data moves between devices by JAX's collectives and lax.ppermute only.
A program may use at most 64 MiB of HBM per device.

```python
import jax
import jax.numpy as jnp
from jax import lax

D = 512
FF = 1536
Q = 8
LEVELS = 8
KERNEL = 7
NFFT = 1280
HOP = 320
BINS = 640
PAD = 480
FRAMES = 8192
RECS = 8
SAMPLES = 2621440


def plant(values, key, least, high):
    spot = [jax.random.randint(jax.random.fold_in(key, axis), (), 0, length) for axis, length in enumerate(values.shape)]
    widest = values.shape.index(max(values.shape))
    neighbour = spot[:widest] + [(spot[widest] + 1) % values.shape[widest]] + spot[widest + 1:]
    return values.at[tuple(spot)].set(least).at[tuple(neighbour)].set(high)


def steps_of(key, extent, shards, smallest, largest):
    factor_of, own = 1.0, jax.random.fold_in(key, 6)
    for dim, shards_of in shards:
        draws = jnp.exp(jax.random.uniform(jax.random.fold_in(own, dim), (shards_of,), jnp.float32, smallest / len(shards), largest / len(shards)))
        factor_of = factor_of * jnp.repeat(draws, extent[dim] // shards_of).reshape([-1 if axis == dim else 1 for axis in range(len(extent))])
    return factor_of


def bell_draw(rng, shape, deviation, bound, shards=(), held_as=jnp.bfloat16):
    result = deviation * jax.random.normal(rng, shape, jnp.float32)
    if shards:
        result = result * steps_of(rng, shape, shards, -0.22, 0.18)
    return jnp.clip(result, -bound, bound).astype(held_as)


def setup_inputs(seed: int = 0) -> dict:
    streams_of = jax.random.split(jax.random.key(seed), 17)
    code_indices = plant(jax.random.randint(streams_of[0], (RECS, FRAMES, Q), 0, LEVELS), jax.random.fold_in(streams_of[0], 1), 0, LEVELS - 1).astype(jnp.int32)
    lengths = plant(jax.random.randint(streams_of[1], (RECS,), FRAMES // 2, FRAMES + 1), jax.random.fold_in(streams_of[1], 1), FRAMES // 2, FRAMES).astype(jnp.int32)
    cotangent = bell_draw(streams_of[2], (RECS, SAMPLES), 1.0, 6.0, ((0, 8), (1, 32)))
    embed_weight = bell_draw(streams_of[3], (Q, D), Q ** -0.5, 2.0, (), jnp.float32)
    embed_bias = bell_draw(streams_of[4], (D,), 0.5, 3.0, (), jnp.float32)
    depth_kernel = bell_draw(streams_of[5], (KERNEL, D), KERNEL ** -0.5, 2.0, (), jnp.float32)
    depth_bias = bell_draw(streams_of[6], (D,), 0.5, 3.0, (), jnp.float32)
    norm_gain = jnp.clip(1.0 + 0.1 * jax.random.normal(streams_of[7], (D,), jnp.float32), 0.5, 1.5)
    norm_bias = bell_draw(streams_of[8], (D,), 0.3, 1.75, (), jnp.float32)
    up_weight = bell_draw(streams_of[9], (D, FF), D ** -0.5, 0.25)
    up_bias = bell_draw(streams_of[10], (FF,), 0.5, 3.0, (), jnp.float32)
    down_weight = bell_draw(streams_of[11], (FF, D), FF ** -0.5, 0.15625)
    down_bias = bell_draw(streams_of[12], (D,), 0.3, 1.75, (), jnp.float32)
    layer_scale = jnp.clip(jax.random.uniform(streams_of[13], (D,), jnp.float32, 0.3, 1.0), 0.3, 1.0)
    head_weight = bell_draw(streams_of[14], (D, 2 * BINS), D ** -0.5, 0.25)
    head_bias = bell_draw(streams_of[15], (2 * BINS,), 0.5, 3.0, (), jnp.float32)
    return dict(code_indices=code_indices, lengths=lengths, cotangent=cotangent, embed_weight=embed_weight, embed_bias=embed_bias, depth_kernel=depth_kernel, depth_bias=depth_bias, norm_gain=norm_gain, norm_bias=norm_bias, up_weight=up_weight, up_bias=up_bias, down_weight=down_weight, down_bias=down_bias, layer_scale=layer_scale, head_weight=head_weight, head_bias=head_bias)


EPSILON = 1e-06

def hann_square(position, fft_size):
    window = 0.5 - 0.5 * jnp.cos(2.0 * jnp.pi / fft_size * position)
    return window * window

def synthesis(fft_size, bin_count):
    sample = jnp.arange(fft_size, dtype=jnp.int32)[:, None]
    frequency = jnp.arange(bin_count, dtype=jnp.int32)[None, :]
    turn_count = (sample * frequency % fft_size).astype(jnp.float32)
    angles = 2.0 * jnp.pi / fft_size * turn_count
    window = 0.5 - 0.5 * jnp.cos(2.0 * jnp.pi / fft_size * sample.astype(jnp.float32))
    factor = jnp.where(frequency == 0, 1.0, 2.0).astype(jnp.float32) * window / fft_size
    real_part = factor * jnp.cos(angles)
    imag_part = jnp.where(frequency == 0, 0.0, -factor * jnp.sin(angles))
    return jnp.concatenate([real_part, imag_part], axis=1).astype(jnp.bfloat16)

def sample_scale(first_sample, sample_count, total_frames, hop_size, fft_size, length):
    pad_size = (fft_size - hop_size) // 2
    sample = first_sample + jnp.arange(sample_count, dtype=jnp.int32)
    block_id = sample // hop_size
    offset = sample - block_id * hop_size + pad_size
    envelope = jnp.zeros((sample_count,), jnp.float32)
    for step_back in range(-2, 3):
        frame_id = block_id - step_back
        inside = offset + step_back * hop_size
        usable = (frame_id >= 0) & (frame_id < total_frames) & (inside >= 0) & (inside < fft_size)
        square = hann_square(inside.astype(jnp.float32), fft_size)
        envelope = envelope + jnp.where(usable, square, 0.0)
    alive_mask = sample < length * hop_size
    return jnp.where(alive_mask, 1.0 / envelope, 0.0)

def layer_norm(conv_out, norm_gain, norm_bias):
    centre = conv_out - lax.optimization_barrier(jnp.mean(conv_out, axis=-1, keepdims=True))
    spread = lax.optimization_barrier(jnp.mean(centre * centre, axis=-1, keepdims=True))
    return centre * lax.rsqrt(spread + EPSILON) * norm_gain + norm_bias

def exact_gelu(hidden_pre):
    return jax.nn.gelu(hidden_pre, approximate=False)

def head_map(logits):
    bin_count = logits.shape[1] // 2
    magnitude = jnp.exp(logits[:, :bin_count])
    phase_angle = logits[:, bin_count:]
    return jnp.concatenate([magnitude * jnp.cos(phase_angle), magnitude * jnp.sin(phase_angle)], axis=1)

def contract_rows(former, latter, precision=None):
    return lax.dot_general(former, latter, (((0,), (0,)), ((), ())), precision=precision, preferred_element_type=jnp.float32)

def contract_cols(former, latter):
    return lax.dot_general(former, latter, (((1,), (1,)), ((), ())), preferred_element_type=jnp.float32)

def recording_grads(code_rows, length, cot_row, table, embed_weight, embed_bias, depth_kernel, depth_bias, norm_gain, norm_bias, up_weight, up_bias, down_weight, down_bias, layer_scale, head_weight, head_bias):
    frame_count = code_rows.shape[0]
    frame_ids = jnp.arange(frame_count, dtype=jnp.int32)
    valid = (frame_ids < length).astype(jnp.float32)
    levels_half = (LEVELS - 1) / 2.0
    values = (code_rows.astype(jnp.float32) - levels_half) / levels_half
    projected = jnp.dot(values, embed_weight, precision=lax.Precision.HIGHEST) + embed_bias
    features = (valid[:, None] * projected).astype(jnp.bfloat16)
    padded = jnp.pad(features, ((3, 3), (0, 0)))
    conv_out = jnp.zeros((frame_count, features.shape[1]), jnp.float32) + depth_bias
    for tap_index in range(KERNEL):
        conv_out = conv_out + depth_kernel[tap_index] * padded[tap_index:tap_index + frame_count].astype(jnp.float32)
    normed, norm_pullback = jax.vjp(layer_norm, conv_out, norm_gain, norm_bias)
    normed_low = normed.astype(jnp.bfloat16)
    hidden_pre = jnp.dot(normed_low, up_weight, preferred_element_type=jnp.float32) + up_bias
    activated, gelu_pullback = jax.vjp(exact_gelu, hidden_pre)
    activated_low = activated.astype(jnp.bfloat16)
    branch = jnp.dot(activated_low, down_weight, preferred_element_type=jnp.float32) + down_bias
    latent = (features.astype(jnp.float32) + layer_scale * branch).astype(jnp.bfloat16)
    logits = jnp.dot(latent, head_weight, preferred_element_type=jnp.float32) + head_bias
    spectrum, head_pullback = jax.vjp(head_map, logits)
    sample_weight = sample_scale(0, frame_count * HOP, frame_count, HOP, NFFT, length)
    sample_grad = (cot_row.astype(jnp.float32) * sample_weight).astype(jnp.bfloat16)
    extended = jnp.pad(sample_grad, (PAD, PAD))
    hop_rows = extended.reshape(frame_count + 3, HOP)
    frame_grad = jnp.concatenate([hop_rows[quarter:quarter + frame_count] for quarter in range(4)], axis=1)
    spec_grad = jnp.dot(frame_grad, table, preferred_element_type=jnp.float32)
    logit_grad = head_pullback(spec_grad)[0]
    logit_low = logit_grad.astype(jnp.bfloat16)
    head_weight_grad = contract_rows(latent, logit_low)
    head_bias_grad = lax.optimization_barrier(jnp.sum(logit_grad, axis=0))
    latent_grad = contract_cols(logit_low, head_weight)
    layer_scale_grad = lax.optimization_barrier(jnp.sum(latent_grad * branch, axis=0))
    branch_grad = layer_scale * latent_grad
    down_bias_grad = lax.optimization_barrier(jnp.sum(branch_grad, axis=0))
    branch_low = branch_grad.astype(jnp.bfloat16)
    down_weight_grad = contract_rows(activated_low, branch_low)
    activated_grad = contract_cols(branch_low, down_weight)
    hidden_grad = gelu_pullback(activated_grad)[0]
    up_bias_grad = lax.optimization_barrier(jnp.sum(hidden_grad, axis=0))
    hidden_low = hidden_grad.astype(jnp.bfloat16)
    up_weight_grad = contract_rows(normed_low, hidden_low)
    normed_grad = contract_cols(hidden_low, up_weight)
    conv_grad, norm_gain_grad, norm_bias_grad = norm_pullback(normed_grad)
    depth_kernel_grad = jnp.stack([lax.optimization_barrier(jnp.sum(conv_grad * padded[tap_index:tap_index + frame_count].astype(jnp.float32), axis=0)) for tap_index in range(KERNEL)], axis=0)
    depth_bias_grad = lax.optimization_barrier(jnp.sum(conv_grad, axis=0))
    conv_rims = jnp.pad(conv_grad, ((3, 3), (0, 0)))
    feature_grad = latent_grad
    for tap_index in range(KERNEL):
        feature_grad = feature_grad + depth_kernel[tap_index] * conv_rims[6 - tap_index:6 - tap_index + frame_count]
    feature_grad = valid[:, None] * feature_grad
    embed_weight_grad = contract_rows(values, feature_grad, lax.Precision.HIGHEST)
    embed_bias_grad = lax.optimization_barrier(jnp.sum(feature_grad, axis=0))
    return (embed_weight_grad, embed_bias_grad, depth_kernel_grad, depth_bias_grad, norm_gain_grad, norm_bias_grad, up_weight_grad, up_bias_grad, down_weight_grad, down_bias_grad, layer_scale_grad, head_weight_grad, head_bias_grad)

def reference(code_indices, lengths, cotangent, embed_weight, embed_bias, depth_kernel, depth_bias, norm_gain, norm_bias, up_weight, up_bias, down_weight, down_bias, layer_scale, head_weight, head_bias):
    table = synthesis(NFFT, BINS)
    totals = None
    for record_index in range(RECS):
        grads = recording_grads(code_indices[record_index], lengths[record_index], cotangent[record_index], table, embed_weight, embed_bias, depth_kernel, depth_bias, norm_gain, norm_bias, up_weight, up_bias, down_weight, down_bias, layer_scale, head_weight, head_bias)
        totals = grads if totals is None else tuple((former + latter for former, latter in zip(totals, grads)))
    return (totals[0], totals[1], totals[2], totals[3], totals[4], totals[5], totals[6], totals[7], totals[8], totals[9], totals[10], totals[11], totals[12])
```

```python
import jax
import jax.numpy as jnp
import numpy as np
from jax import lax
from jax.experimental import pallas as pl
from jax.experimental.pallas import tpu as pltpu
from jax.sharding import PartitionSpec as P

D = 512
FF = 1536
Q = 8
KERNEL = 7
NFFT = 1280
HOP = 320
BINS = 640
PAD = 480
EPSILON = 1e-06
HALF = 3.5

FRAMES = 256
PAIRS = FRAMES // 2
ROWS = FRAMES + 16
LEFT = 24
SUB = 72
TAB = 1472
f32 = jnp.float32
bf16 = jnp.bfloat16


def tables():
    n = np.arange(16)[:, None]
    k = np.arange(BINS)[None, :]
    turn = 2.0 * np.pi / NFFT
    out = np.zeros((40, BINS), np.float64)
    out[0:16] = np.cos(turn * (n * k % NFFT))
    out[16:32] = np.sin(turn * (n * k % NFFT))
    out[32] = np.cos(turn * (16 * k[0] % NFFT))
    out[33] = np.sin(turn * (16 * k[0] % NFFT))
    out[34] = np.where(k[0] == 0, 1.0, 2.0) / NFFT
    out[35] = np.where(k[0] == 0, 0.0, -2.0) / NFFT
    return out.astype(np.float32)


def edges():
    def square(i):
        return np.where((i >= 0) & (i < NFFT), (0.5 - 0.5 * np.cos(2.0 * np.pi / NFFT * i)) ** 2, 0.0)

    s = np.arange(512)
    first = sum(square(s + PAD - HOP * t) for t in range(4))
    last = sum(square(s - 32 + HOP * t) for t in range(1, 5))
    out = np.zeros((8, 128), np.float64)
    out[0:4] = (1.0 / first).reshape(4, 128)
    out[4:8] = (1.0 / last).reshape(4, 128)
    return out.astype(np.float32)


def dot(a, b):
    return lax.dot_general(a, b, (((1,), (0,)), ((), ())), preferred_element_type=f32)


def dot_rows(a, b):
    return lax.dot_general(a, b, (((0,), (0,)), ((), ())), preferred_element_type=f32)


def dot_cols(a, b):
    return lax.dot_general(a, b, (((1,), (1,)), ((), ())), preferred_element_type=f32)


def sine_cosine(p):
    k = jnp.round(p * np.float32(2.0 / np.pi))
    r = p - k * np.float32(1.5703125)
    r = r - k * np.float32(4.837512969970703125e-4)
    r = r - k * np.float32(7.54978995489188216e-8)
    z = r * r
    s = r + r * z * (np.float32(-1.6666654611e-1) + z * (np.float32(8.3321608736e-3) + z * np.float32(-1.9515295891e-4)))
    c = 1.0 - 0.5 * z + z * z * (
        np.float32(4.166664568298827e-2) + z * (np.float32(-1.388731625493765e-3) + z * np.float32(2.443315711809948e-5))
    )
    q = k.astype(jnp.int32)
    odd = (q & 1) == 1
    sine = jnp.where(odd, c, s)
    cosine = jnp.where(odd, s, c)
    sine = jnp.where((q & 2) == 2, -sine, sine)
    cosine = jnp.where(((q + 1) & 2) == 2, -cosine, cosine)
    return sine, cosine


def split3(w):
    hi = w.astype(bf16)
    rest = w - hi.astype(f32)
    mid = rest.astype(bf16)
    low = (rest - mid.astype(f32)).astype(bf16)
    return hi, mid, low


def local_kernel(
    pos, codes, cot, left, right, embed_w, embed_b, depth_k, depth_b, gain, bias, up_w, up_b, down_w, down_b,
    scale, head_w, head_b, trig, edge, out,
    tab, feat, conv, cgrad, latg, samp, pair_rows, spec_in, xhat, rstd, normed, hid, dgelu, act, branch, latent, re, im,
    logit_low, low, big, spec, lg, row_sums, sums, tiles,
):
    first_frame, length = pos[0], pos[1]
    last_frame = pos[2]

    tab[0:96, :] = jnp.zeros((96, NFFT), bf16)
    tab[1376:TAB, :] = jnp.zeros((TAB - 1376, NFFT), bf16)
    cs, sn = trig[32:33, :], trig[33:34, :]
    real_row, imag_row = trig[34:35, :], trig[35:36, :]

    def table_step(i, carry):
        c, s = carry
        window = 0.5 - 0.5 * c[:, 1:2]
        at = pl.multiple_of(96 + i * 16, 16)
        tab[pl.ds(at, 16), 0:BINS] = (c * (window * real_row)).astype(bf16)
        tab[pl.ds(at, 16), BINS:] = (s * (window * imag_row)).astype(bf16)
        return c * cs - s * sn, s * cs + c * sn

    lax.fori_loop(0, NFFT // 16, table_step, (trig[0:16, :], trig[16:32, :]))

    w_hi, w_mid, w_low = split3(embed_w[...])

    def project(c):
        c = c.astype(bf16)
        return (dot_rows(c, w_hi) + dot_rows(c, w_mid) + dot_rows(c, w_low)) * np.float32(1.0 / HALF) + embed_b[...]

    own_codes = codes[...].astype(f32) - HALF
    feat[0:16, :] = jnp.zeros((16, D), f32)
    feat[16 + FRAMES :, :] = jnp.zeros((feat.shape[0] - 16 - FRAMES, D), f32)
    feat[16 : 16 + FRAMES, :] = project(own_codes)
    feat[8:16, :] = project(left[LEFT:, :].astype(f32) - HALF)[120:128, :]
    feat[16 + FRAMES : 24 + FRAMES, :] = project(right[LEFT:, :].astype(f32) - HALF)[0:8, :]

    def mask_step(i, _):
        at = pl.multiple_of(8 + i * 8, 8)
        frame = first_frame + (at - 16) + lax.broadcasted_iota(jnp.int32, (8, D), 0)
        keep = (frame >= 0) & (frame < length)
        feat[pl.ds(at, 8), :] = jnp.where(keep, feat[pl.ds(at, 8), :], 0.0).astype(bf16).astype(f32)
        return 0

    lax.fori_loop(0, (FRAMES + 16) // 8, mask_step, 0)

    taps = [depth_k[j : j + 1, :] for j in range(KERNEL)]
    total = jnp.broadcast_to(depth_b[...], (FRAMES + 16, D))
    for j in range(KERNEL):
        total = total + taps[j] * feat[5 + j : 5 + j + FRAMES + 16, :]
    conv[...] = total

    def to_rows(ref, base, dst):
        dst[0:FRAMES, :] = ref[base : base + FRAMES, :]
        dst[FRAMES : FRAMES + 8, :] = ref[base - 8 : base, :]
        dst[FRAMES + 8 :, :] = ref[base + FRAMES : base + FRAMES + 8, :]

    to_rows(conv, 8, xhat)

    def norm_step(i, _):
        at = pl.ds(pl.multiple_of(i * 16, 16), 16)
        x = xhat[at, :]
        centre = x - jnp.mean(x, axis=1, keepdims=True)
        r = lax.rsqrt(jnp.mean(centre * centre, axis=1, keepdims=True) + EPSILON)
        x = centre * r
        xhat[at, :] = x
        rstd[at, :] = jnp.broadcast_to(r, (16, 128))
        normed[at, :] = (x * gain[...] + bias[...]).astype(bf16)
        return 0

    lax.fori_loop(0, ROWS // 16, norm_step, 0)

    hid[...] = dot(normed[...], up_w[...])

    def gelu_step(i, _):
        at = pl.ds(pl.multiple_of(i * 16, 16), 16)
        x = hid[at, :] + up_b[...]
        cdf = 0.5 + 0.5 * lax.erf(x * np.float32(0.7071067811865476))
        act[at, :] = (x * cdf).astype(bf16)
        dgelu[at, :] = cdf + x * (jnp.exp(-0.5 * x * x) * np.float32(0.3989422804014327))
        return 0

    lax.fori_loop(0, ROWS // 16, gelu_step, 0)

    branch[...] = dot(act[...], down_w[...]) + down_b[...]
    to_rows(feat, 16, lg)
    latent[...] = (lg[...] + scale[...] * branch[...]).astype(bf16)

    big[0:ROWS, 0:NFFT] = dot(latent[...], head_w[...])

    def head_step(i, _):
        at = pl.ds(pl.multiple_of(i * 16, 16), 16)
        magnitude = jnp.exp(big[at, 0:BINS] + head_b[:, 0:BINS])
        sine, cosine = sine_cosine(big[at, BINS:NFFT] + head_b[:, BINS:])
        re[at, :] = magnitude * cosine
        im[at, :] = magnitude * sine
        return 0

    lax.fori_loop(0, ROWS // 16, head_step, 0)

    samp[0:LEFT, :] = left[0:LEFT, :].astype(f32)
    samp[LEFT : LEFT + 640, :] = cot[...]
    samp[LEFT + 640 :, :] = right[0:LEFT, :].astype(f32)
    start = first_frame * HOP
    limit = length * HOP

    def sample_step(i, _):
        at = pl.multiple_of(i * 8, 8)
        row = at - LEFT + lax.broadcasted_iota(jnp.int32, (8, 128), 0)
        s = start + row * 128 + lax.broadcasted_iota(jnp.int32, (8, 128), 1)
        x = samp[pl.ds(at, 8), :] * np.float32(2.0 / 3.0)
        samp[pl.ds(at, 8), :] = jnp.where(s < limit, x, 0.0)
        return 0

    def fix(at, values):
        row = at - LEFT + lax.broadcasted_iota(jnp.int32, (4, 128), 0)
        s = start + row * 128 + lax.broadcasted_iota(jnp.int32, (4, 128), 1)
        samp[at : at + 4, :] = jnp.where(s < limit, cot[at - LEFT : at - LEFT + 4, :] * values, 0.0)

    lax.fori_loop(0, (LEFT * 2 + 640) // 8, sample_step, 0)

    @pl.when(first_frame == 0)
    def _():
        fix(LEFT, edge[0:4, :])

    @pl.when(first_frame + FRAMES == last_frame)
    def _():
        fix(LEFT + 636, edge[4:8, :])

    for d in range(3):
        for k in range(5):
            column = (d * 5 + k) * 128
            base = LEFT + (d - 1) * 5 + k
            spec_in[0:PAIRS, column : column + 128] = samp[pl.ds(base, PAIRS, stride=5), :].astype(bf16)
            pair_rows[0:2, column : column + 128] = samp[pl.ds(base - 10, 2, stride=5), :]
            pair_rows[2:4, column : column + 128] = samp[pl.ds(base + 640, 2, stride=5), :]
    pair_rows[4:16, :] = jnp.zeros((12, 1920), f32)
    spec_in[PAIRS : PAIRS + 16, :] = pair_rows[...].astype(bf16)

    even = dot(spec_in[:, 128:1536], tab[64:1472, :])
    odd = dot(spec_in[:, 384:1792], tab[0:1408, :])
    for t in range(10):
        column = slice(128 * t, 128 * t + 128)
        spec[t, FRAMES:, :] = jnp.zeros((16, 128), f32)
        for part, parity in ((even, 0), (odd, 1)):
            spec[t, pl.ds(parity, PAIRS, stride=2), :] = part[0:PAIRS, column]
            spec[t, pl.ds(FRAMES + 4 + parity, 4, stride=2), :] = part[PAIRS : PAIRS + 4, column]

    def logit_grad_of(at):
        das, dps = [], []
        for t in range(5):
            column = slice(128 * t, 128 * t + 128)
            g_re, g_im = spec[t, at, :], spec[t + 5, at, :]
            r, m = re[at, column], im[at, column]
            da = g_re * r + g_im * m
            dp = g_im * r - g_re * m
            logit_low[at, column] = da.astype(bf16)
            logit_low[at, BINS + 128 * t : BINS + 128 * t + 128] = dp.astype(bf16)
            das.append(da)
            dps.append(dp)
        return jnp.concatenate(das, axis=1), jnp.concatenate(dps, axis=1)

    def logit_step(i, carry):
        da, dp = logit_grad_of(pl.ds(pl.multiple_of(i * 16, 16), 16))
        return carry[0] + da[0:8] + da[8:16], carry[1] + dp[0:8] + dp[8:16]

    zero = jnp.zeros((8, BINS), f32)
    da, dp = lax.fori_loop(0, FRAMES // 16, logit_step, (zero, zero))
    logit_grad_of(pl.ds(FRAMES, 16))
    head_sum = jnp.concatenate([jnp.sum(da, axis=0, keepdims=True), jnp.sum(dp, axis=0, keepdims=True)], axis=1)
    for t in range(10):
        tiles[16 + t : 17 + t, :] = head_sum[:, 128 * t : 128 * t + 128]

    latg[...] = dot_cols(logit_low[...], head_w[...])

    def scatter(columns, height, row):
        def step(f, _):
            z, yl, c = f // 4, (f // 2) % 2, f % 2
            for j in range(columns):
                for h in range(height // 8):
                    o = row + j * height + h * 8
                    at = pl.multiple_of(f * height + h * 8, 8)
                    out[c, yl, o // SUB, z, o % SUB : o % SUB + 8, :] = big[pl.ds(at, 8), 128 * j : 128 * j + 128].astype(bf16)
            return 0

        lax.fori_loop(0, 32, step, 0)

    big[0:D, 0:NFFT] = dot_rows(latent[0:FRAMES, :], logit_low[0:FRAMES, :])
    scatter(10, 16, 192)

    def latent_step(i, carry):
        at = pl.ds(pl.multiple_of(i * 16, 16), 16)
        g = latg[at, :]
        low[at, :] = (scale[...] * g).astype(bf16)
        b = g * branch[at, :]
        return carry[0] + b[0:8] + b[8:16], carry[1] + g[0:8] + g[8:16]

    zero = jnp.zeros((8, D), f32)
    scale_sum, latent_sum = lax.fori_loop(0, FRAMES // 16, latent_step, (zero, zero))
    low[FRAMES:, :] = (scale[...] * latg[FRAMES:, :]).astype(bf16)
    sums[20:21, :] = jnp.sum(scale_sum, axis=0, keepdims=True)
    sums[19:20, :] = jnp.sum(latent_sum, axis=0, keepdims=True) * scale[...]

    big[:, 0:D] = dot_rows(act[0:FRAMES, :], low[0:FRAMES, :])
    scatter(4, 48, 352)

    hid[...] = dot_cols(low[...], down_w[...])

    def hidden_grad_of(at):
        g = hid[at, :] * dgelu[at, :]
        act[at, :] = g.astype(bf16)
        return g

    def hidden_step(i, carry):
        g = hidden_grad_of(pl.ds(pl.multiple_of(i * 16, 16), 16))
        return carry + g[0:8] + g[8:16]

    up_sum = lax.fori_loop(0, FRAMES // 16, hidden_step, jnp.zeros((8, FF), f32))
    hidden_grad_of(pl.ds(FRAMES, 16))
    up_sum = jnp.sum(up_sum, axis=0, keepdims=True)
    for t in range(12):
        tiles[t : t + 1, :] = up_sum[:, 128 * t : 128 * t + 128]

    big[0:D, 0:FF] = dot_rows(normed[0:FRAMES, :], act[0:FRAMES, :])
    scatter(12, 16, 0)

    lg[...] = dot_cols(act[...], up_w[...])

    def norm_grad_of(at):
        g, x = lg[at, :], xhat[at, :]
        dx = g * gain[...]
        m1 = jnp.mean(dx, axis=1, keepdims=True)
        m2 = jnp.mean(dx * x, axis=1, keepdims=True)
        lg[at, :] = rstd[at, 0:1] * (dx - m1 - x * m2)
        return g, g * x

    def norm_grad_step(i, carry):
        g, gx = norm_grad_of(pl.ds(pl.multiple_of(i * 16, 16), 16))
        return carry[0] + g[0:8] + g[8:16], carry[1] + gx[0:8] + gx[8:16]

    bias_sum, gain_sum = lax.fori_loop(0, FRAMES // 16, norm_grad_step, (zero, zero))
    norm_grad_of(pl.ds(FRAMES, 16))
    sums[17:18, :] = jnp.sum(gain_sum, axis=0, keepdims=True)
    sums[18:19, :] = jnp.sum(bias_sum, axis=0, keepdims=True)

    i = lax.broadcasted_iota(jnp.int32, (16, D), 0)
    frame = jnp.where(i < 8, i - 8, i + (FRAMES - 8)) + first_frame
    inside = (frame >= 0) & (frame < last_frame)
    edge_rows = jnp.where(inside, lg[FRAMES:, :], 0.0)

    cgrad[0:8, :] = edge_rows[0:8]
    cgrad[8 : 8 + FRAMES, :] = lg[0:FRAMES, :]
    cgrad[8 + FRAMES :, :] = edge_rows[8:16]

    own = cgrad[8 : 8 + FRAMES, :]
    sums[16:17, :] = jnp.sum(own, axis=0, keepdims=True)
    total = latg[0:FRAMES, :]
    for j in range(KERNEL):
        sums[9 + j : 10 + j, :] = jnp.sum(own * feat[13 + j : 13 + j + FRAMES, :], axis=0, keepdims=True)
        total = total + taps[j] * cgrad[11 - j : 11 - j + FRAMES, :]
    frame = first_frame + lax.broadcasted_iota(jnp.int32, (FRAMES, D), 0)
    total = jnp.where(frame < length, total, 0.0)
    sums[8:9, :] = jnp.sum(total, axis=0, keepdims=True)
    hi, mid, rest = split3(total)
    own_low = own_codes.astype(bf16)
    sums[0:8, :] = (dot(own_low, hi) + dot(own_low, mid) + dot(own_low, rest)) * np.float32(1.0 / HALF)
    sums[21:24, :] = jnp.zeros((3, D), f32)

    def small_step(f, _):
        z, yl, c = f // 4, (f // 2) % 2, f % 2
        row_sums[...] = jnp.zeros((8, 128), f32)
        row_sums[0:2, :] = tiles[pl.ds((48 * f) // 128, 2), :]
        row_sums[2:4, :] = tiles[pl.ds(16 + (40 * f) // 128, 2), :]
        out[c, yl, 7, z, 64:72, :] = row_sums[...].astype(bf16)
        return 0

    tiles[12:16, :] = jnp.zeros((4, 128), f32)
    tiles[26:32, :] = jnp.zeros((6, 128), f32)
    lax.fori_loop(0, 32, small_step, 0)
    for f in range(32):
        column = 128 * (f // 8)
        out[f % 2, (f // 2) % 2, 7, f // 4, 40:64, :] = sums[:, column : column + 128].astype(bf16)


def local_grads(pos, codes, cot, left, right, weights):
    vmem = pltpu.VMEM
    scratch = [
        vmem((TAB, NFFT), bf16),
        vmem((FRAMES + 32, D), f32),
        vmem((FRAMES + 16, D), f32),
        vmem((FRAMES + 16, D), f32),
        vmem((ROWS, D), f32),
        vmem((640 + 2 * LEFT, 128), f32),
        vmem((16, 1920), f32),
        vmem((PAIRS + 16, 1920), bf16),
        vmem((ROWS, D), f32),
        vmem((ROWS, 128), f32),
        vmem((ROWS, D), bf16),
        vmem((ROWS, FF), f32),
        vmem((ROWS, FF), f32),
        vmem((ROWS, FF), bf16),
        vmem((ROWS, D), f32),
        vmem((ROWS, D), bf16),
        vmem((ROWS, BINS), f32),
        vmem((ROWS, BINS), f32),
        vmem((ROWS, NFFT), bf16),
        vmem((ROWS, D), bf16),
        vmem((FF, FF), f32),
        vmem((10, ROWS, 128), f32),
        vmem((ROWS, D), f32),
        vmem((8, 128), f32),
        vmem((24, D), f32),
        vmem((32, 128), f32),
    ]
    whole = pl.BlockSpec(memory_space=pltpu.VMEM)
    arrays = [codes, cot, left, right, *weights, jnp.asarray(tables()), jnp.asarray(edges())]
    return pl.pallas_call(
        local_kernel,
        out_shape=jax.ShapeDtypeStruct((2, 2, 8, 8, SUB, 128), bf16),
        in_specs=[pl.BlockSpec(memory_space=pltpu.SMEM)] + [whole] * len(arrays),
        out_specs=whole,
        scratch_shapes=scratch,
        compiler_params=pltpu.CompilerParams(vmem_limit_bytes=56 * 1024 * 1024),
        name="local_grads",
    )(pos, *arrays)


def unpack_kernel(pos, t, up_g, head_g, down_g, embed_w, embed_b, depth_k, vectors, up_b, head_b):
    f = pos[0]

    def tile(o):
        return t[o // SUB, o % SUB : o % SUB + 8, :]

    for columns, height, row, ref in ((12, 16, 0, up_g), (10, 16, 192, head_g), (4, 48, 352, down_g)):
        for j in range(columns):
            for h in range(height // 8):
                ref[h * 8 : h * 8 + 8, 128 * j : 128 * j + 128] = tile(row + j * height + h * 8)
    shift = 16 * (f % 8)
    back = lax.rem(128 - shift, 128)

    def rolled(x, by):
        return pltpu.roll(x, by, 1)

    embed_w[...] = rolled(tile(544), back)[:, 0:16]
    second = rolled(tile(552), back)
    third = rolled(tile(560), back)
    embed_b[...] = second[0:1, 0:16]
    depth_k[...] = second[1:8, 0:16]
    vectors[...] = third[0:8, 0:16]
    last = tile(568)
    lane = lax.broadcasted_iota(jnp.int32, (1, 128), 1)
    for row, width, ref in ((0, 48, up_b), (2, 40, head_b)):
        shift = lax.rem(width * f, 128)
        back = lax.rem(128 - shift, 128)
        moved = rolled(last, back)
        joined = jnp.where(lane < 128 - shift, moved[row : row + 1, :], moved[row + 1 : row + 2, :])
        ref[...] = joined[:, 0:width]


def unpack(pos, t):
    def shape(*s):
        return jax.ShapeDtypeStruct(s, f32)

    whole = pl.BlockSpec(memory_space=pltpu.VMEM)
    return pl.pallas_call(
        unpack_kernel,
        out_shape=(
            shape(16, FF), shape(16, NFFT), shape(48, D), shape(8, 16), shape(1, 16), shape(7, 16), shape(8, 16), shape(1, 48), shape(1, 40),
        ),
        in_specs=[pl.BlockSpec(memory_space=pltpu.SMEM), whole],
        out_specs=(whole,) * 9,
        name="unpack",
    )(pos, t)


AXES = ("frame", "rec")


def index_of(z, yl, c, yh, x):
    return ((z * 2 + yl) * 2 + c) * 8 + yh * 4 + x


def groups_over(which):
    sizes = dict(z=8, yl=2, c=2, yh=2, x=4)
    kept = [n for n in sizes if n not in which]

    def walk(names, fixed):
        if not names:
            return [fixed]
        return [r for v in range(sizes[names[0]]) for r in walk(names[1:], {**fixed, names[0]: v})]

    return [[index_of(**g) for g in walk(list(which), fixed)] for fixed in walk(kept, {})]


def exchange(array, which):
    return lax.all_to_all(array, AXES, split_axis=0, concat_axis=0, axis_index_groups=groups_over(which), tiled=True)


def summed(array):
    return jnp.sum(array.astype(f32), axis=0)


def reduce_all(packed):
    both = exchange(packed.reshape(2, -1, 128), ("c",))
    half = summed(both).astype(bf16).reshape(16, 8 * SUB, 128)
    part = summed(exchange(half, ("yl", "yh", "x"))).astype(bf16).reshape(8, SUB, 128)
    mine = summed(exchange(part, ("z",)))
    return lax.all_to_all(jnp.broadcast_to(mine, (8, SUB, 128)), "rec", split_axis=0, concat_axis=0, tiled=True)


def body(code_indices, lengths, cotangent, *weights):
    count = lax.axis_size("frame")
    me = lax.axis_index("frame")
    codes = code_indices[0].T
    samples = cotangent[0].astype(f32).reshape(640, 128)
    low = samples.astype(bf16)
    codes_low = codes.astype(bf16)
    forward = [(i, i + 1) for i in range(count - 1)]
    backward = [(b, a) for a, b in forward]
    left = lax.ppermute(jnp.concatenate([low[640 - LEFT :], codes_low[:, FRAMES - 128 :]]), "frame", forward)
    right = lax.ppermute(jnp.concatenate([low[:LEFT], codes_low[:, :128]]), "frame", backward)
    pos = jnp.stack([me * FRAMES, lengths[0], count * FRAMES]).astype(jnp.int32)
    flat = [w if w.ndim == 2 else w[None] for w in weights]
    packed = local_grads(pos, codes, samples, left, right, flat)
    t = reduce_all(packed)
    up_g, head_g, down_g, embed_w, embed_b, depth_k, vectors, up_b, head_b = unpack(me.astype(jnp.int32)[None], t)
    depth_b, gain, bias, down_b, scale = (vectors[i] for i in range(5))
    return (
        embed_w, embed_b[0], depth_k, depth_b, gain, bias, up_g, up_b[0], down_g, down_b, scale, head_g, head_b[0],
    )


def solution(mesh):
    return jax.shard_map(
        body,
        mesh=mesh,
        in_specs=(P("rec", "frame", None), P("rec"), P("rec", "frame")) + (P(),) * 13,
        out_specs=(
            P(None, "frame"), P("frame"), P(None, "frame"), P("frame"), P("frame"), P("frame"), P("frame", None),
            P("frame"), P("frame", None), P("frame"), P("frame"), P("frame", None), P("frame"),
        ),
        check_vma=False,
    )
```

```python
import jax
import jax.numpy as jnp
import numpy as np
from jax import lax
from jax.experimental import pallas as pl
from jax.experimental.pallas import tpu as pltpu
from jax.sharding import PartitionSpec as P

D = 512
FF = 1536
Q = 8
KERNEL = 7
NFFT = 1280
HOP = 320
BINS = 640
PAD = 480
EPSILON = 1e-06
HALF = 3.5

FRAMES = 256
PAIRS = FRAMES // 2
ROWS = FRAMES + 16
LEFT = 24
SUB = 72
TAB = 1472
f32 = jnp.float32
bf16 = jnp.bfloat16


def tables():
    n = np.arange(16)[:, None]
    k = np.arange(BINS)[None, :]
    turn = 2.0 * np.pi / NFFT
    out = np.zeros((40, BINS), np.float64)
    out[0:16] = np.cos(turn * (n * k % NFFT))
    out[16:32] = np.sin(turn * (n * k % NFFT))
    out[32] = np.cos(turn * (16 * k[0] % NFFT))
    out[33] = np.sin(turn * (16 * k[0] % NFFT))
    out[34] = np.where(k[0] == 0, 1.0, 2.0) / NFFT
    out[35] = np.where(k[0] == 0, 0.0, -2.0) / NFFT
    return out.astype(np.float32)


def edges():
    def square(i):
        return np.where((i >= 0) & (i < NFFT), (0.5 - 0.5 * np.cos(2.0 * np.pi / NFFT * i)) ** 2, 0.0)

    s = np.arange(512)
    first = sum(square(s + PAD - HOP * t) for t in range(4))
    last = sum(square(s - 32 + HOP * t) for t in range(1, 5))
    out = np.zeros((8, 128), np.float64)
    out[0:4] = (1.0 / first).reshape(4, 128)
    out[4:8] = (1.0 / last).reshape(4, 128)
    return out.astype(np.float32)


def dot(a, b):
    return lax.dot_general(a, b, (((1,), (0,)), ((), ())), preferred_element_type=f32)


def dot_rows(a, b):
    return lax.dot_general(a, b, (((0,), (0,)), ((), ())), preferred_element_type=f32)


def dot_cols(a, b):
    return lax.dot_general(a, b, (((1,), (1,)), ((), ())), preferred_element_type=f32)


def sine_cosine(p):
    k = jnp.round(p * np.float32(2.0 / np.pi))
    r = p - k * np.float32(1.5703125)
    r = r - k * np.float32(4.837512969970703125e-4)
    r = r - k * np.float32(7.54978995489188216e-8)
    z = r * r
    s = r + r * z * (np.float32(-1.6666654611e-1) + z * (np.float32(8.3321608736e-3) + z * np.float32(-1.9515295891e-4)))
    c = 1.0 - 0.5 * z + z * z * (
        np.float32(4.166664568298827e-2) + z * (np.float32(-1.388731625493765e-3) + z * np.float32(2.443315711809948e-5))
    )
    q = k.astype(jnp.int32)
    odd = (q & 1) == 1
    sine = jnp.where(odd, c, s)
    cosine = jnp.where(odd, s, c)
    sine = jnp.where((q & 2) == 2, -sine, sine)
    cosine = jnp.where(((q + 1) & 2) == 2, -cosine, cosine)
    return sine, cosine


def split3(w):
    hi = w.astype(bf16)
    rest = w - hi.astype(f32)
    mid = rest.astype(bf16)
    low = (rest - mid.astype(f32)).astype(bf16)
    return hi, mid, low


def local_kernel(
    pos, codes, cot, left, right, embed_w, embed_b, depth_k, depth_b, gain, bias, up_w, up_b, down_w, down_b,
    scale, head_w, head_b, trig, edge, keep, send,
    tab, feat, conv, cgrad, latg, samp, pair_rows, spec_in, xhat, rstd, normed, hid, dgelu, act, branch, latent, re, im,
    logit_low, low, big, spec, lg, row_sums, sums, tiles, tall, rows,
):
    first_frame, length = pos[0], pos[1]
    last_frame = pos[2]
    core = pos[3]

    for t in range(FF // 128):
        rows[0:1, 128 * t : 128 * t + 128] = up_b[t : t + 1, :]
    for t in range(NFFT // 128):
        rows[1:2, 128 * t : 128 * t + 128] = head_b[t : t + 1, :]
    up_row, head_row = rows[0:1, :], rows[1:2, 0:NFFT]

    tab[0:96, :] = jnp.zeros((96, NFFT), bf16)
    tab[1376:TAB, :] = jnp.zeros((TAB - 1376, NFFT), bf16)
    cs, sn = trig[32:33, :], trig[33:34, :]
    real_row, imag_row = trig[34:35, :], trig[35:36, :]

    def table_step(i, carry):
        c, s = carry
        window = 0.5 - 0.5 * c[:, 1:2]
        at = pl.multiple_of(96 + i * 16, 16)
        tab[pl.ds(at, 16), 0:BINS] = (c * (window * real_row)).astype(bf16)
        tab[pl.ds(at, 16), BINS:] = (s * (window * imag_row)).astype(bf16)
        return c * cs - s * sn, s * cs + c * sn

    lax.fori_loop(0, NFFT // 16, table_step, (trig[0:16, :], trig[16:32, :]))

    w_hi, w_mid, w_low = split3(embed_w[...])

    def project(c):
        c = c.astype(bf16)
        return (dot_rows(c, w_hi) + dot_rows(c, w_mid) + dot_rows(c, w_low)) * np.float32(1.0 / HALF) + embed_b[...]

    own_codes = codes[...].astype(f32) - HALF
    feat[0:16, :] = jnp.zeros((16, D), f32)
    feat[16 + FRAMES :, :] = jnp.zeros((feat.shape[0] - 16 - FRAMES, D), f32)
    feat[16 : 16 + FRAMES, :] = project(own_codes)
    feat[8:16, :] = project(left[LEFT:, :].astype(f32) - HALF)[120:128, :]
    feat[16 + FRAMES : 24 + FRAMES, :] = project(right[LEFT:, :].astype(f32) - HALF)[0:8, :]

    def mask_step(i, _):
        at = pl.multiple_of(8 + i * 8, 8)
        frame = first_frame + (at - 16) + lax.broadcasted_iota(jnp.int32, (8, D), 0)
        keep = (frame >= 0) & (frame < length)
        feat[pl.ds(at, 8), :] = jnp.where(keep, feat[pl.ds(at, 8), :], 0.0).astype(bf16).astype(f32)
        return 0

    lax.fori_loop(0, (FRAMES + 16) // 8, mask_step, 0)

    taps = [depth_k[j : j + 1, :] for j in range(KERNEL)]
    total = jnp.broadcast_to(depth_b[...], (FRAMES + 16, D))
    for j in range(KERNEL):
        total = total + taps[j] * feat[5 + j : 5 + j + FRAMES + 16, :]
    conv[...] = total

    def to_rows(ref, base, dst):
        dst[0:FRAMES, :] = ref[base : base + FRAMES, :]
        dst[FRAMES : FRAMES + 8, :] = ref[base - 8 : base, :]
        dst[FRAMES + 8 :, :] = ref[base + FRAMES : base + FRAMES + 8, :]

    to_rows(conv, 8, xhat)

    def norm_step(i, _):
        at = pl.ds(pl.multiple_of(i * 16, 16), 16)
        x = xhat[at, :]
        centre = x - jnp.mean(x, axis=1, keepdims=True)
        r = lax.rsqrt(jnp.mean(centre * centre, axis=1, keepdims=True) + EPSILON)
        x = centre * r
        xhat[at, :] = x
        rstd[at, :] = jnp.broadcast_to(r, (16, 128))
        normed[at, :] = (x * gain[...] + bias[...]).astype(bf16)
        return 0

    lax.fori_loop(0, ROWS // 16, norm_step, 0)

    hid[...] = dot(normed[...], up_w[...])

    def gelu_step(i, _):
        at = pl.ds(pl.multiple_of(i * 16, 16), 16)
        x = hid[at, :] + up_row
        cdf = 0.5 + 0.5 * lax.erf(x * np.float32(0.7071067811865476))
        act[at, :] = (x * cdf).astype(bf16)
        dgelu[at, :] = cdf + x * (jnp.exp(-0.5 * x * x) * np.float32(0.3989422804014327))
        return 0

    lax.fori_loop(0, ROWS // 16, gelu_step, 0)

    branch[...] = dot(act[...], down_w[...]) + down_b[...]
    to_rows(feat, 16, lg)
    latent[...] = (lg[...] + scale[...] * branch[...]).astype(bf16)

    big[0:ROWS, 0:NFFT] = dot(latent[...], head_w[...])

    def head_step(i, _):
        at = pl.ds(pl.multiple_of(i * 16, 16), 16)
        magnitude = jnp.exp(big[at, 0:BINS] + head_row[:, 0:BINS])
        sine, cosine = sine_cosine(big[at, BINS:NFFT] + head_row[:, BINS:])
        re[at, :] = magnitude * cosine
        im[at, :] = magnitude * sine
        return 0

    lax.fori_loop(0, ROWS // 16, head_step, 0)

    samp[0:LEFT, :] = left[0:LEFT, :].astype(f32)
    samp[LEFT : LEFT + 640, :] = cot[...]
    samp[LEFT + 640 :, :] = right[0:LEFT, :].astype(f32)
    start = first_frame * HOP
    limit = length * HOP

    def sample_step(i, _):
        at = pl.multiple_of(i * 8, 8)
        row = at - LEFT + lax.broadcasted_iota(jnp.int32, (8, 128), 0)
        s = start + row * 128 + lax.broadcasted_iota(jnp.int32, (8, 128), 1)
        x = samp[pl.ds(at, 8), :] * np.float32(2.0 / 3.0)
        samp[pl.ds(at, 8), :] = jnp.where(s < limit, x, 0.0)
        return 0

    def fix(at, values):
        row = at - LEFT + lax.broadcasted_iota(jnp.int32, (4, 128), 0)
        s = start + row * 128 + lax.broadcasted_iota(jnp.int32, (4, 128), 1)
        samp[at : at + 4, :] = jnp.where(s < limit, cot[at - LEFT : at - LEFT + 4, :] * values, 0.0)

    lax.fori_loop(0, (LEFT * 2 + 640) // 8, sample_step, 0)

    @pl.when(first_frame == 0)
    def _():
        fix(LEFT, edge[0:4, :])

    @pl.when(first_frame + FRAMES == last_frame)
    def _():
        fix(LEFT + 636, edge[4:8, :])

    for d in range(3):
        for k in range(5):
            column = (d * 5 + k) * 128
            base = LEFT + (d - 1) * 5 + k
            spec_in[0:PAIRS, column : column + 128] = samp[pl.ds(base, PAIRS, stride=5), :].astype(bf16)
            pair_rows[0:2, column : column + 128] = samp[pl.ds(base - 10, 2, stride=5), :]
            pair_rows[2:4, column : column + 128] = samp[pl.ds(base + 640, 2, stride=5), :]
    pair_rows[4:16, :] = jnp.zeros((12, 1920), f32)
    spec_in[PAIRS : PAIRS + 16, :] = pair_rows[...].astype(bf16)

    even = dot(spec_in[:, 128:1536], tab[64:1472, :])
    odd = dot(spec_in[:, 384:1792], tab[0:1408, :])
    for t in range(10):
        column = slice(128 * t, 128 * t + 128)
        spec[t, FRAMES:, :] = jnp.zeros((16, 128), f32)
        for part, parity in ((even, 0), (odd, 1)):
            spec[t, pl.ds(parity, PAIRS, stride=2), :] = part[0:PAIRS, column]
            spec[t, pl.ds(FRAMES + 4 + parity, 4, stride=2), :] = part[PAIRS : PAIRS + 4, column]

    def logit_grad_of(at):
        das, dps = [], []
        for t in range(5):
            column = slice(128 * t, 128 * t + 128)
            g_re, g_im = spec[t, at, :], spec[t + 5, at, :]
            r, m = re[at, column], im[at, column]
            da = g_re * r + g_im * m
            dp = g_im * r - g_re * m
            logit_low[at, column] = da.astype(bf16)
            logit_low[at, BINS + 128 * t : BINS + 128 * t + 128] = dp.astype(bf16)
            das.append(da)
            dps.append(dp)
        return jnp.concatenate(das, axis=1), jnp.concatenate(dps, axis=1)

    def logit_step(i, carry):
        da, dp = logit_grad_of(pl.ds(pl.multiple_of(i * 16, 16), 16))
        return carry[0] + da[0:8] + da[8:16], carry[1] + dp[0:8] + dp[8:16]

    zero = jnp.zeros((8, BINS), f32)
    da, dp = lax.fori_loop(0, FRAMES // 16, logit_step, (zero, zero))
    logit_grad_of(pl.ds(FRAMES, 16))
    head_sum = jnp.concatenate([jnp.sum(da, axis=0, keepdims=True), jnp.sum(dp, axis=0, keepdims=True)], axis=1)
    for t in range(10):
        tiles[16 + t : 17 + t, :] = head_sum[:, 128 * t : 128 * t + 128]

    latg[...] = dot_cols(logit_low[...], head_w[...])

    def scatter(big_ref, columns, height, row):
        def step(p, _):
            z, yl = p // 2, p % 2
            for ref, f in ((keep, 2 * p + core), (send, 2 * p + 1 - core)):
                for j in range(columns):
                    for h in range(height // 8):
                        o = row + j * height + h * 8
                        at = pl.multiple_of(f * height + h * 8, 8)
                        value = big_ref[pl.ds(at, 8), 128 * j : 128 * j + 128].astype(bf16)
                        ref[yl, o // SUB, z, o % SUB : o % SUB + 8, :] = value
            return 0

        lax.fori_loop(0, 16, step, 0)

    big[0:D, 0:NFFT] = dot_rows(latent[0:FRAMES, :], logit_low[0:FRAMES, :])
    scatter(big, 10, 16, 192)

    def latent_step(i, carry):
        at = pl.ds(pl.multiple_of(i * 16, 16), 16)
        g = latg[at, :]
        low[at, :] = (scale[...] * g).astype(bf16)
        b = g * branch[at, :]
        return carry[0] + b[0:8] + b[8:16], carry[1] + g[0:8] + g[8:16]

    zero = jnp.zeros((8, D), f32)
    scale_sum, latent_sum = lax.fori_loop(0, FRAMES // 16, latent_step, (zero, zero))
    low[FRAMES:, :] = (scale[...] * latg[FRAMES:, :]).astype(bf16)
    sums[20:21, :] = jnp.sum(scale_sum, axis=0, keepdims=True)
    sums[19:20, :] = jnp.sum(latent_sum, axis=0, keepdims=True) * scale[...]

    tall[...] = dot_rows(act[0:FRAMES, :], low[0:FRAMES, :])
    scatter(tall, 4, 48, 352)

    hid[...] = dot_cols(low[...], down_w[...])

    def hidden_grad_of(at):
        g = hid[at, :] * dgelu[at, :]
        act[at, :] = g.astype(bf16)
        return g

    def hidden_step(i, carry):
        g = hidden_grad_of(pl.ds(pl.multiple_of(i * 16, 16), 16))
        return carry + g[0:8] + g[8:16]

    up_sum = lax.fori_loop(0, FRAMES // 16, hidden_step, jnp.zeros((8, FF), f32))
    hidden_grad_of(pl.ds(FRAMES, 16))
    up_sum = jnp.sum(up_sum, axis=0, keepdims=True)
    for t in range(12):
        tiles[t : t + 1, :] = up_sum[:, 128 * t : 128 * t + 128]

    big[0:D, 0:FF] = dot_rows(normed[0:FRAMES, :], act[0:FRAMES, :])
    scatter(big, 12, 16, 0)

    lg[...] = dot_cols(act[...], up_w[...])

    def norm_grad_of(at):
        g, x = lg[at, :], xhat[at, :]
        dx = g * gain[...]
        m1 = jnp.mean(dx, axis=1, keepdims=True)
        m2 = jnp.mean(dx * x, axis=1, keepdims=True)
        lg[at, :] = rstd[at, 0:1] * (dx - m1 - x * m2)
        return g, g * x

    def norm_grad_step(i, carry):
        g, gx = norm_grad_of(pl.ds(pl.multiple_of(i * 16, 16), 16))
        return carry[0] + g[0:8] + g[8:16], carry[1] + gx[0:8] + gx[8:16]

    bias_sum, gain_sum = lax.fori_loop(0, FRAMES // 16, norm_grad_step, (zero, zero))
    norm_grad_of(pl.ds(FRAMES, 16))
    sums[17:18, :] = jnp.sum(gain_sum, axis=0, keepdims=True)
    sums[18:19, :] = jnp.sum(bias_sum, axis=0, keepdims=True)

    i = lax.broadcasted_iota(jnp.int32, (16, D), 0)
    frame = jnp.where(i < 8, i - 8, i + (FRAMES - 8)) + first_frame
    inside = (frame >= 0) & (frame < last_frame)
    edge_rows = jnp.where(inside, lg[FRAMES:, :], 0.0)

    cgrad[0:8, :] = edge_rows[0:8]
    cgrad[8 : 8 + FRAMES, :] = lg[0:FRAMES, :]
    cgrad[8 + FRAMES :, :] = edge_rows[8:16]

    own = cgrad[8 : 8 + FRAMES, :]
    sums[16:17, :] = jnp.sum(own, axis=0, keepdims=True)
    total = latg[0:FRAMES, :]
    for j in range(KERNEL):
        sums[9 + j : 10 + j, :] = jnp.sum(own * feat[13 + j : 13 + j + FRAMES, :], axis=0, keepdims=True)
        total = total + taps[j] * cgrad[11 - j : 11 - j + FRAMES, :]
    frame = first_frame + lax.broadcasted_iota(jnp.int32, (FRAMES, D), 0)
    total = jnp.where(frame < length, total, 0.0)
    sums[8:9, :] = jnp.sum(total, axis=0, keepdims=True)
    hi, mid, rest = split3(total)
    own_low = own_codes.astype(bf16)
    sums[0:8, :] = (dot(own_low, hi) + dot(own_low, mid) + dot(own_low, rest)) * np.float32(1.0 / HALF)
    sums[21:24, :] = jnp.zeros((3, D), f32)

    tiles[12:16, :] = jnp.zeros((4, 128), f32)
    tiles[26:32, :] = jnp.zeros((6, 128), f32)
    row_sums[...] = jnp.zeros((8, 128), f32)

    def small_step(p, _):
        z, yl = p // 2, p % 2
        for ref, f in ((keep, 2 * p + core), (send, 2 * p + 1 - core)):
            row_sums[0:2, :] = tiles[pl.ds((48 * f) // 128, 2), :]
            row_sums[2:4, :] = tiles[pl.ds(16 + (40 * f) // 128, 2), :]
            ref[yl, 7, z, 64:72, :] = row_sums[...].astype(bf16)
        return 0

    lax.fori_loop(0, 16, small_step, 0)
    for p in range(16):
        column = 128 * (p // 4)
        part = sums[:, column : column + 128].astype(bf16)
        keep[p % 2, 7, p // 2, 40:64, :] = part
        send[p % 2, 7, p // 2, 40:64, :] = part


def local_grads(pos, codes, cot, left, right, weights):
    vmem = pltpu.VMEM
    scratch = [
        vmem((TAB, NFFT), bf16),
        vmem((FRAMES + 32, D), f32),
        vmem((FRAMES + 16, D), f32),
        vmem((FRAMES + 16, D), f32),
        vmem((ROWS, D), f32),
        vmem((640 + 2 * LEFT, 128), f32),
        vmem((16, 1920), f32),
        vmem((PAIRS + 16, 1920), bf16),
        vmem((ROWS, D), f32),
        vmem((ROWS, 128), f32),
        vmem((ROWS, D), bf16),
        vmem((ROWS, FF), f32),
        vmem((ROWS, FF), f32),
        vmem((ROWS, FF), bf16),
        vmem((ROWS, D), f32),
        vmem((ROWS, D), bf16),
        vmem((ROWS, BINS), f32),
        vmem((ROWS, BINS), f32),
        vmem((ROWS, NFFT), bf16),
        vmem((ROWS, D), bf16),
        vmem((D, FF), f32),
        vmem((10, ROWS, 128), f32),
        vmem((ROWS, D), f32),
        vmem((8, 128), f32),
        vmem((24, D), f32),
        vmem((32, 128), f32),
        vmem((FF, D), f32),
        vmem((8, FF), f32),
    ]
    whole = pl.BlockSpec(memory_space=pltpu.VMEM)
    arrays = [codes, cot, left, right, *weights, jnp.asarray(tables()), jnp.asarray(edges())]
    return pl.pallas_call(
        local_kernel,
        out_shape=(jax.ShapeDtypeStruct((2, 8, 8, SUB, 128), bf16),) * 2,
        in_specs=[pl.BlockSpec(memory_space=pltpu.SMEM)] + [whole] * len(arrays),
        out_specs=(whole, whole),
        scratch_shapes=scratch,
        compiler_params=pltpu.CompilerParams(vmem_limit_bytes=42 * 1024 * 1024),
        name="local_grads",
    )(pos, *arrays)


def unpack_kernel(pos, t, up_g, head_g, down_g, embed_w, embed_b, depth_k, vectors, up_b, head_b):
    f = pos[0]

    def tile(o):
        return t[o // SUB, o % SUB : o % SUB + 8, :]

    for columns, height, row, ref in ((12, 16, 0, up_g), (10, 16, 192, head_g), (4, 48, 352, down_g)):
        for j in range(columns):
            for h in range(height // 8):
                ref[h * 8 : h * 8 + 8, 128 * j : 128 * j + 128] = tile(row + j * height + h * 8)
    shift = 16 * (f % 8)
    back = lax.rem(128 - shift, 128)

    def rolled(x, by):
        return pltpu.roll(x, by, 1)

    embed_w[...] = rolled(tile(544), back)[:, 0:16]
    second = rolled(tile(552), back)
    third = rolled(tile(560), back)
    embed_b[...] = second[0:1, 0:16]
    depth_k[...] = second[1:8, 0:16]
    vectors[...] = third[0:8, 0:16]
    last = tile(568)
    lane = lax.broadcasted_iota(jnp.int32, (1, 128), 1)
    for row, width, ref in ((0, 48, up_b), (2, 40, head_b)):
        shift = lax.rem(width * f, 128)
        back = lax.rem(128 - shift, 128)
        moved = rolled(last, back)
        joined = jnp.where(lane < 128 - shift, moved[row : row + 1, :], moved[row + 1 : row + 2, :])
        ref[...] = joined[:, 0:width]


def unpack(pos, t):
    def shape(*s):
        return jax.ShapeDtypeStruct(s, f32)

    whole = pl.BlockSpec(memory_space=pltpu.VMEM)
    return pl.pallas_call(
        unpack_kernel,
        out_shape=(
            shape(16, FF), shape(16, NFFT), shape(48, D), shape(8, 16), shape(1, 16), shape(7, 16), shape(8, 16), shape(1, 48), shape(1, 40),
        ),
        in_specs=[pl.BlockSpec(memory_space=pltpu.SMEM), whole],
        out_specs=(whole,) * 9,
        name="unpack",
    )(pos, t)


AXES = ("frame", "rec")


def index_of(z, yl, c, yh, x):
    return ((z * 2 + yl) * 2 + c) * 8 + yh * 4 + x


def groups_over(which):
    sizes = dict(z=8, yl=2, c=2, yh=2, x=4)
    kept = [n for n in sizes if n not in which]

    def walk(names, fixed):
        if not names:
            return [fixed]
        return [r for v in range(sizes[names[0]]) for r in walk(names[1:], {**fixed, names[0]: v})]

    return [[index_of(**g) for g in walk(list(which), fixed)] for fixed in walk(kept, {})]


def exchange(array, which):
    return lax.all_to_all(array, AXES, split_axis=0, concat_axis=0, axis_index_groups=groups_over(which), tiled=True)


def summed(array):
    return jnp.sum(array.astype(f32), axis=0)


def reduce_all(keep, send):
    pairs = groups_over(("c",))
    other = lax.ppermute(send, AXES, [(a, b) for a, b in pairs] + [(b, a) for a, b in pairs])
    half = (keep.astype(f32) + other.astype(f32)).astype(bf16).reshape(16, 8 * SUB, 128)
    part = summed(exchange(half, ("yl", "yh", "x"))).astype(bf16).reshape(8, SUB, 128)
    mine = summed(exchange(part, ("z",)))
    return lax.all_to_all(jnp.broadcast_to(mine, (8, SUB, 128)), "rec", split_axis=0, concat_axis=0, tiled=True)


def body(code_indices, lengths, cotangent, *weights):
    count = lax.axis_size("frame")
    me = lax.axis_index("frame")
    codes = code_indices[0].T
    samples = cotangent[0].astype(f32).reshape(640, 128)
    low = samples.astype(bf16)
    codes_low = codes.astype(bf16)
    forward = [(i, i + 1) for i in range(count - 1)]
    backward = [(b, a) for a, b in forward]
    left = lax.ppermute(jnp.concatenate([low[640 - LEFT :], codes_low[:, FRAMES - 128 :]]), "frame", forward)
    right = lax.ppermute(jnp.concatenate([low[:LEFT], codes_low[:, :128]]), "frame", backward)
    pos = jnp.stack([me * FRAMES, lengths[0], count * FRAMES, me % 2]).astype(jnp.int32)
    flat = [w if w.ndim == 2 else w[None] if w.size == D else w.reshape(-1, 128) for w in weights]
    t = reduce_all(*local_grads(pos, codes, samples, left, right, flat))
    up_g, head_g, down_g, embed_w, embed_b, depth_k, vectors, up_b, head_b = unpack(me.astype(jnp.int32)[None], t)
    depth_b, gain, bias, down_b, scale = (vectors[i] for i in range(5))
    return (
        embed_w, embed_b[0], depth_k, depth_b, gain, bias, up_g, up_b[0], down_g, down_b, scale, head_g, head_b[0],
    )


def solution(mesh):
    return jax.shard_map(
        body,
        mesh=mesh,
        in_specs=(P("rec", "frame", None), P("rec"), P("rec", "frame")) + (P(),) * 13,
        out_specs=(
            P(None, "frame"), P("frame"), P(None, "frame"), P("frame"), P("frame"), P("frame"), P("frame", None),
            P("frame"), P("frame", None), P("frame"), P("frame"), P("frame", None), P("frame"),
        ),
        check_vma=False,
    )
```

```python
import jax
import jax.numpy as jnp
import numpy as np
from jax import lax
from jax.experimental import pallas as pl
from jax.experimental.pallas import tpu as pltpu
from jax.sharding import PartitionSpec as P

D = 512
FF = 1536
Q = 8
KERNEL = 7
NFFT = 1280
HOP = 320
BINS = 640
PAD = 480
EPSILON = 1e-06
HALF = 3.5

FRAMES = 256
PAIRS = FRAMES // 2
ROWS = FRAMES + 16
LEFT = 24
SUB = 72
TAB = 1472
f32 = jnp.float32
bf16 = jnp.bfloat16


def tables():
    n = np.arange(16)[:, None]
    k = np.arange(BINS)[None, :]
    turn = 2.0 * np.pi / NFFT
    out = np.zeros((40, BINS), np.float64)
    out[0:16] = np.cos(turn * (n * k % NFFT))
    out[16:32] = np.sin(turn * (n * k % NFFT))
    out[32] = np.cos(turn * (16 * k[0] % NFFT))
    out[33] = np.sin(turn * (16 * k[0] % NFFT))
    out[34] = np.where(k[0] == 0, 1.0, 2.0) / NFFT
    out[35] = np.where(k[0] == 0, 0.0, -2.0) / NFFT
    return out.astype(np.float32)


def edges():
    def square(i):
        return np.where((i >= 0) & (i < NFFT), (0.5 - 0.5 * np.cos(2.0 * np.pi / NFFT * i)) ** 2, 0.0)

    s = np.arange(512)
    first = sum(square(s + PAD - HOP * t) for t in range(4))
    last = sum(square(s - 32 + HOP * t) for t in range(1, 5))
    out = np.zeros((8, 128), np.float64)
    out[0:4] = (1.0 / first).reshape(4, 128)
    out[4:8] = (1.0 / last).reshape(4, 128)
    return out.astype(np.float32)


def dot(a, b):
    return lax.dot_general(a, b, (((1,), (0,)), ((), ())), preferred_element_type=f32)


def dot_rows(a, b):
    return lax.dot_general(a, b, (((0,), (0,)), ((), ())), preferred_element_type=f32)


def dot_cols(a, b):
    return lax.dot_general(a, b, (((1,), (1,)), ((), ())), preferred_element_type=f32)


def sine_cosine(p):
    k = jnp.round(p * np.float32(2.0 / np.pi))
    r = p - k * np.float32(1.5703125)
    r = r - k * np.float32(4.837512969970703125e-4)
    r = r - k * np.float32(7.54978995489188216e-8)
    z = r * r
    s = r + r * z * (np.float32(-1.6666654611e-1) + z * (np.float32(8.3321608736e-3) + z * np.float32(-1.9515295891e-4)))
    c = 1.0 - 0.5 * z + z * z * (
        np.float32(4.166664568298827e-2) + z * (np.float32(-1.388731625493765e-3) + z * np.float32(2.443315711809948e-5))
    )
    q = k.astype(jnp.int32)
    odd = (q & 1) == 1
    sine = jnp.where(odd, c, s)
    cosine = jnp.where(odd, s, c)
    sine = jnp.where((q & 2) == 2, -sine, sine)
    cosine = jnp.where(((q + 1) & 2) == 2, -cosine, cosine)
    return sine, cosine


def split3(w):
    hi = w.astype(bf16)
    rest = w - hi.astype(f32)
    mid = rest.astype(bf16)
    low = (rest - mid.astype(f32)).astype(bf16)
    return hi, mid, low


def setup_kernel(*refs):
    count = (len(refs) - 4) // 2
    sources, trig_far, outs = refs[:count], refs[count], refs[count + 1 : -3]
    tab, trig, sems = refs[-3:]
    first = pltpu.make_async_copy(trig_far, trig, sems.at[count])
    copies = [pltpu.make_async_copy(a, b, sems.at[i]) for i, (a, b) in enumerate(zip(sources, outs))]
    first.start()
    for copy in copies:
        copy.start()

    tab[0:96, :] = jnp.zeros((96, NFFT), bf16)
    tab[1376:TAB, :] = jnp.zeros((TAB - 1376, NFFT), bf16)
    first.wait()
    cs, sn = trig[32:33, :], trig[33:34, :]
    real_row, imag_row = trig[34:35, :], trig[35:36, :]

    def table_step(i, carry):
        c, s = carry
        window = 0.5 - 0.5 * c[:, 1:2]
        at = pl.multiple_of(96 + i * 16, 16)
        tab[pl.ds(at, 16), 0:BINS] = (c * (window * real_row)).astype(bf16)
        tab[pl.ds(at, 16), BINS:] = (s * (window * imag_row)).astype(bf16)
        return c * cs - s * sn, s * cs + c * sn

    lax.fori_loop(0, NFFT // 16, table_step, (trig[0:16, :], trig[16:32, :]))
    for copy in copies:
        copy.wait()


def setup(arrays):
    whole = pl.BlockSpec(memory_space=pltpu.VMEM)
    return pl.pallas_call(
        setup_kernel,
        out_shape=tuple(jax.ShapeDtypeStruct(a.shape, a.dtype) for a in arrays) + (jax.ShapeDtypeStruct((TAB, NFFT), bf16),),
        in_specs=[pl.BlockSpec(memory_space=pltpu.HBM)] * (len(arrays) + 1),
        out_specs=(whole,) * (len(arrays) + 1),
        scratch_shapes=[pltpu.VMEM((40, BINS), f32), pltpu.SemaphoreType.DMA((len(arrays) + 1,))],
        compiler_params=pltpu.CompilerParams(vmem_limit_bytes=16 * 1024 * 1024),
        name="setup",
    )(*[pltpu.with_memory_space_constraint(a, pltpu.HBM) for a in (*arrays, jnp.asarray(tables()))])


def local_kernel(
    pos, cot, left, right, codes, embed_w, embed_b, depth_k, depth_b, gain, bias, up_w, up_b, down_w, down_b,
    scale, head_w, head_b, edge, tab, keep, send,
    feat, conv, cgrad, latg, samp, pair_rows, spec_in, xhat, rstd, normed, hid, dgelu, act, branch, latent, re, im,
    logit_low, low, big, spec, lg, row_sums, sums, tiles, tall, rows,
):
    first_frame, length = pos[0], pos[1]
    last_frame = pos[2]
    core = pos[3]

    for t in range(FF // 128):
        rows[0:1, 128 * t : 128 * t + 128] = up_b[t : t + 1, :]
    for t in range(NFFT // 128):
        rows[1:2, 128 * t : 128 * t + 128] = head_b[t : t + 1, :]
    up_row, head_row = rows[0:1, :], rows[1:2, 0:NFFT]

    w_hi, w_mid, w_low = split3(embed_w[...])

    def project(c):
        c = c.astype(bf16)
        return (dot_rows(c, w_hi) + dot_rows(c, w_mid) + dot_rows(c, w_low)) * np.float32(1.0 / HALF) + embed_b[...]

    own_codes = codes[...].astype(f32) - HALF
    feat[0:16, :] = jnp.zeros((16, D), f32)
    feat[16 + FRAMES :, :] = jnp.zeros((feat.shape[0] - 16 - FRAMES, D), f32)
    feat[16 : 16 + FRAMES, :] = project(own_codes)
    feat[8:16, :] = project(left[LEFT:, :].astype(f32) - HALF)[120:128, :]
    feat[16 + FRAMES : 24 + FRAMES, :] = project(right[LEFT:, :].astype(f32) - HALF)[0:8, :]

    def mask_step(i, _):
        at = pl.multiple_of(8 + i * 8, 8)
        frame = first_frame + (at - 16) + lax.broadcasted_iota(jnp.int32, (8, D), 0)
        keep = (frame >= 0) & (frame < length)
        feat[pl.ds(at, 8), :] = jnp.where(keep, feat[pl.ds(at, 8), :], 0.0).astype(bf16).astype(f32)
        return 0

    lax.fori_loop(0, (FRAMES + 16) // 8, mask_step, 0)

    taps = [depth_k[j : j + 1, :] for j in range(KERNEL)]
    total = jnp.broadcast_to(depth_b[...], (FRAMES + 16, D))
    for j in range(KERNEL):
        total = total + taps[j] * feat[5 + j : 5 + j + FRAMES + 16, :]
    conv[...] = total

    def to_rows(ref, base, dst):
        dst[0:FRAMES, :] = ref[base : base + FRAMES, :]
        dst[FRAMES : FRAMES + 8, :] = ref[base - 8 : base, :]
        dst[FRAMES + 8 :, :] = ref[base + FRAMES : base + FRAMES + 8, :]

    to_rows(conv, 8, xhat)

    x = xhat[...]
    centre = x - jnp.mean(x, axis=1, keepdims=True)
    r = lax.rsqrt(jnp.mean(centre * centre, axis=1, keepdims=True) + EPSILON)
    x = centre * r
    xhat[...] = x
    rstd[...] = jnp.broadcast_to(r, (ROWS, 128))
    normed[...] = (x * gain[...] + bias[...]).astype(bf16)

    hid[...] = dot(normed[...], up_w[...])

    def gelu_step(i, _):
        at = pl.ds(pl.multiple_of(i * 16, 16), 16)
        x = hid[at, :] + up_row
        cdf = 0.5 + 0.5 * lax.erf(x * np.float32(0.7071067811865476))
        act[at, :] = (x * cdf).astype(bf16)
        dgelu[at, :] = cdf + x * (jnp.exp(-0.5 * x * x) * np.float32(0.3989422804014327))
        return 0

    lax.fori_loop(0, ROWS // 16, gelu_step, 0)

    branch[...] = dot(act[...], down_w[...]) + down_b[...]
    to_rows(feat, 16, lg)
    latent[...] = (lg[...] + scale[...] * branch[...]).astype(bf16)

    big[0:ROWS, 0:NFFT] = dot(latent[...], head_w[...])

    def head_step(i, _):
        at = pl.ds(pl.multiple_of(i * 16, 16), 16)
        magnitude = jnp.exp(big[at, 0:BINS] + head_row[:, 0:BINS])
        sine, cosine = sine_cosine(big[at, BINS:NFFT] + head_row[:, BINS:])
        re[at, :] = magnitude * cosine
        im[at, :] = magnitude * sine
        return 0

    lax.fori_loop(0, ROWS // 16, head_step, 0)

    samp[0:LEFT, :] = left[0:LEFT, :].astype(f32)
    samp[LEFT : LEFT + 640, :] = cot[...]
    samp[LEFT + 640 :, :] = right[0:LEFT, :].astype(f32)
    start = first_frame * HOP
    limit = length * HOP

    def sample_step(i, _):
        at = pl.multiple_of(i * 8, 8)
        row = at - LEFT + lax.broadcasted_iota(jnp.int32, (8, 128), 0)
        s = start + row * 128 + lax.broadcasted_iota(jnp.int32, (8, 128), 1)
        x = samp[pl.ds(at, 8), :] * np.float32(2.0 / 3.0)
        samp[pl.ds(at, 8), :] = jnp.where(s < limit, x, 0.0)
        return 0

    def fix(at, values):
        row = at - LEFT + lax.broadcasted_iota(jnp.int32, (4, 128), 0)
        s = start + row * 128 + lax.broadcasted_iota(jnp.int32, (4, 128), 1)
        samp[at : at + 4, :] = jnp.where(s < limit, cot[at - LEFT : at - LEFT + 4, :] * values, 0.0)

    lax.fori_loop(0, (LEFT * 2 + 640) // 8, sample_step, 0)

    @pl.when(first_frame == 0)
    def _():
        fix(LEFT, edge[0:4, :])

    @pl.when(first_frame + FRAMES == last_frame)
    def _():
        fix(LEFT + 636, edge[4:8, :])

    for d in range(3):
        for k in range(5):
            column = (d * 5 + k) * 128
            base = LEFT + (d - 1) * 5 + k
            spec_in[0:PAIRS, column : column + 128] = samp[pl.ds(base, PAIRS, stride=5), :].astype(bf16)
            pair_rows[0:2, column : column + 128] = samp[pl.ds(base - 10, 2, stride=5), :]
            pair_rows[2:4, column : column + 128] = samp[pl.ds(base + 640, 2, stride=5), :]
    pair_rows[4:16, :] = jnp.zeros((12, 1920), f32)
    spec_in[PAIRS : PAIRS + 16, :] = pair_rows[...].astype(bf16)

    even = dot(spec_in[:, 128:1536], tab[64:1472, :])
    odd = dot(spec_in[:, 384:1792], tab[0:1408, :])
    for t in range(10):
        column = slice(128 * t, 128 * t + 128)
        spec[t, FRAMES:, :] = jnp.zeros((16, 128), f32)
        for part, parity in ((even, 0), (odd, 1)):
            spec[t, pl.ds(parity, PAIRS, stride=2), :] = part[0:PAIRS, column]
            spec[t, pl.ds(FRAMES + 4 + parity, 4, stride=2), :] = part[PAIRS : PAIRS + 4, column]

    def logit_grad_of(at):
        das, dps = [], []
        for t in range(5):
            column = slice(128 * t, 128 * t + 128)
            g_re, g_im = spec[t, at, :], spec[t + 5, at, :]
            r, m = re[at, column], im[at, column]
            da = g_re * r + g_im * m
            dp = g_im * r - g_re * m
            logit_low[at, column] = da.astype(bf16)
            logit_low[at, BINS + 128 * t : BINS + 128 * t + 128] = dp.astype(bf16)
            das.append(da)
            dps.append(dp)
        return jnp.concatenate(das, axis=1), jnp.concatenate(dps, axis=1)

    def logit_step(i, carry):
        da, dp = logit_grad_of(pl.ds(pl.multiple_of(i * 16, 16), 16))
        return carry[0] + da[0:8] + da[8:16], carry[1] + dp[0:8] + dp[8:16]

    zero = jnp.zeros((8, BINS), f32)
    da, dp = lax.fori_loop(0, FRAMES // 16, logit_step, (zero, zero))
    logit_grad_of(pl.ds(FRAMES, 16))
    head_sum = jnp.concatenate([jnp.sum(da, axis=0, keepdims=True), jnp.sum(dp, axis=0, keepdims=True)], axis=1)
    for t in range(10):
        tiles[16 + t : 17 + t, :] = head_sum[:, 128 * t : 128 * t + 128]

    latg[...] = dot_cols(logit_low[...], head_w[...])

    def scatter(big_ref, columns, height, row):
        def step(p, _):
            z, yl = p // 2, p % 2
            for ref, f in ((keep, 2 * p + core), (send, 2 * p + 1 - core)):
                for j in range(columns):
                    for h in range(height // 8):
                        o = row + j * height + h * 8
                        at = pl.multiple_of(f * height + h * 8, 8)
                        value = big_ref[pl.ds(at, 8), 128 * j : 128 * j + 128].astype(bf16)
                        ref[yl, o // SUB, z, o % SUB : o % SUB + 8, :] = value
            return 0

        lax.fori_loop(0, 16, step, 0)

    big[0:D, 0:NFFT] = dot_rows(latent[0:FRAMES, :], logit_low[0:FRAMES, :])
    scatter(big, 10, 16, 192)

    def latent_step(i, carry):
        at = pl.ds(pl.multiple_of(i * 16, 16), 16)
        g = latg[at, :]
        low[at, :] = (scale[...] * g).astype(bf16)
        b = g * branch[at, :]
        return carry[0] + b[0:8] + b[8:16], carry[1] + g[0:8] + g[8:16]

    zero = jnp.zeros((8, D), f32)
    scale_sum, latent_sum = lax.fori_loop(0, FRAMES // 16, latent_step, (zero, zero))
    low[FRAMES:, :] = (scale[...] * latg[FRAMES:, :]).astype(bf16)
    sums[20:21, :] = jnp.sum(scale_sum, axis=0, keepdims=True)
    sums[19:20, :] = jnp.sum(latent_sum, axis=0, keepdims=True) * scale[...]

    tall[...] = dot_rows(act[0:FRAMES, :], low[0:FRAMES, :])
    scatter(tall, 4, 48, 352)

    hid[...] = dot_cols(low[...], down_w[...])

    def hidden_grad_of(at):
        g = hid[at, :] * dgelu[at, :]
        act[at, :] = g.astype(bf16)
        return g

    def hidden_step(i, carry):
        g = hidden_grad_of(pl.ds(pl.multiple_of(i * 16, 16), 16))
        return carry + g[0:8] + g[8:16]

    up_sum = lax.fori_loop(0, FRAMES // 16, hidden_step, jnp.zeros((8, FF), f32))
    hidden_grad_of(pl.ds(FRAMES, 16))
    up_sum = jnp.sum(up_sum, axis=0, keepdims=True)
    for t in range(12):
        tiles[t : t + 1, :] = up_sum[:, 128 * t : 128 * t + 128]

    big[0:D, 0:FF] = dot_rows(normed[0:FRAMES, :], act[0:FRAMES, :])
    scatter(big, 12, 16, 0)

    lg[...] = dot_cols(act[...], up_w[...])

    g, x = lg[...], xhat[...]
    dx = g * gain[...]
    m1 = jnp.mean(dx, axis=1, keepdims=True)
    m2 = jnp.mean(dx * x, axis=1, keepdims=True)
    lg[...] = rstd[:, 0:1] * (dx - m1 - x * m2)
    sums[17:18, :] = jnp.sum(g[0:FRAMES] * x[0:FRAMES], axis=0, keepdims=True)
    sums[18:19, :] = jnp.sum(g[0:FRAMES], axis=0, keepdims=True)

    i = lax.broadcasted_iota(jnp.int32, (16, D), 0)
    frame = jnp.where(i < 8, i - 8, i + (FRAMES - 8)) + first_frame
    inside = (frame >= 0) & (frame < last_frame)
    edge_rows = jnp.where(inside, lg[FRAMES:, :], 0.0)

    cgrad[0:8, :] = edge_rows[0:8]
    cgrad[8 : 8 + FRAMES, :] = lg[0:FRAMES, :]
    cgrad[8 + FRAMES :, :] = edge_rows[8:16]

    own = cgrad[8 : 8 + FRAMES, :]
    sums[16:17, :] = jnp.sum(own, axis=0, keepdims=True)
    total = latg[0:FRAMES, :]
    for j in range(KERNEL):
        sums[9 + j : 10 + j, :] = jnp.sum(own * feat[13 + j : 13 + j + FRAMES, :], axis=0, keepdims=True)
        total = total + taps[j] * cgrad[11 - j : 11 - j + FRAMES, :]
    frame = first_frame + lax.broadcasted_iota(jnp.int32, (FRAMES, D), 0)
    total = jnp.where(frame < length, total, 0.0)
    sums[8:9, :] = jnp.sum(total, axis=0, keepdims=True)
    hi, mid, rest = split3(total)
    own_low = own_codes.astype(bf16)
    sums[0:8, :] = (dot(own_low, hi) + dot(own_low, mid) + dot(own_low, rest)) * np.float32(1.0 / HALF)
    sums[21:24, :] = jnp.zeros((3, D), f32)

    tiles[12:16, :] = jnp.zeros((4, 128), f32)
    tiles[26:32, :] = jnp.zeros((6, 128), f32)
    row_sums[...] = jnp.zeros((8, 128), f32)

    def small_step(p, _):
        z, yl = p // 2, p % 2
        for ref, f in ((keep, 2 * p + core), (send, 2 * p + 1 - core)):
            row_sums[0:2, :] = tiles[pl.ds((48 * f) // 128, 2), :]
            row_sums[2:4, :] = tiles[pl.ds(16 + (40 * f) // 128, 2), :]
            ref[yl, 7, z, 64:72, :] = row_sums[...].astype(bf16)
        return 0

    lax.fori_loop(0, 16, small_step, 0)
    for p in range(16):
        column = 128 * (p // 4)
        part = sums[:, column : column + 128].astype(bf16)
        keep[p % 2, 7, p // 2, 40:64, :] = part
        send[p % 2, 7, p // 2, 40:64, :] = part


def local_grads(pos, cot, left, right, ready):
    vmem = pltpu.VMEM
    scratch = [
        vmem((FRAMES + 32, D), f32),
        vmem((FRAMES + 16, D), f32),
        vmem((FRAMES + 16, D), f32),
        vmem((ROWS, D), f32),
        vmem((640 + 2 * LEFT, 128), f32),
        vmem((16, 1920), f32),
        vmem((PAIRS + 16, 1920), bf16),
        vmem((ROWS, D), f32),
        vmem((ROWS, 128), f32),
        vmem((ROWS, D), bf16),
        vmem((ROWS, FF), f32),
        vmem((ROWS, FF), f32),
        vmem((ROWS, FF), bf16),
        vmem((ROWS, D), f32),
        vmem((ROWS, D), bf16),
        vmem((ROWS, BINS), f32),
        vmem((ROWS, BINS), f32),
        vmem((ROWS, NFFT), bf16),
        vmem((ROWS, D), bf16),
        vmem((D, FF), f32),
        vmem((10, ROWS, 128), f32),
        vmem((ROWS, D), f32),
        vmem((8, 128), f32),
        vmem((24, D), f32),
        vmem((32, 128), f32),
        vmem((FF, D), f32),
        vmem((8, FF), f32),
    ]
    whole = pl.BlockSpec(memory_space=pltpu.VMEM)
    arrays = [cot, left, right, *ready]
    return pl.pallas_call(
        local_kernel,
        out_shape=(jax.ShapeDtypeStruct((2, 8, 8, SUB, 128), bf16),) * 2,
        in_specs=[pl.BlockSpec(memory_space=pltpu.SMEM)] + [whole] * len(arrays),
        out_specs=(whole, whole),
        scratch_shapes=scratch,
        compiler_params=pltpu.CompilerParams(vmem_limit_bytes=38 * 1024 * 1024),
        name="local_grads",
    )(pos, *arrays)


def unpack_kernel(pos, t, up_g, head_g, down_g, embed_w, embed_b, depth_k, up_b, head_b, *vectors):
    f = pos[0]

    def tile(o):
        return t[o // SUB, o % SUB : o % SUB + 8, :].astype(f32)

    for columns, height, row, ref in ((12, 16, 0, up_g), (10, 16, 192, head_g), (4, 48, 352, down_g)):
        for j in range(columns):
            for h in range(height // 8):
                ref[h * 8 : h * 8 + 8, 128 * j : 128 * j + 128] = tile(row + j * height + h * 8)
    shift = 16 * (f % 8)
    back = lax.rem(128 - shift, 128)

    def rolled(x, by):
        return pltpu.roll(x, by, 1)

    embed_w[...] = rolled(tile(544), back)[:, 0:16]
    second = rolled(tile(552), back)
    third = rolled(tile(560), back)
    embed_b[...] = second[0:1, 0:16]
    depth_k[...] = second[1:8, 0:16]
    for i, ref in enumerate(vectors):
        ref[...] = third[i : i + 1, 0:16]
    last = tile(568)
    lane = lax.broadcasted_iota(jnp.int32, (1, 128), 1)
    for row, width, ref in ((0, 48, up_b), (2, 40, head_b)):
        shift = lax.rem(width * f, 128)
        back = lax.rem(128 - shift, 128)
        moved = rolled(last, back)
        joined = jnp.where(lane < 128 - shift, moved[row : row + 1, :], moved[row + 1 : row + 2, :])
        ref[...] = joined[:, 0:width]


def unpack(pos, t):
    def shape(*s):
        return jax.ShapeDtypeStruct(s, f32)

    whole = pl.BlockSpec(memory_space=pltpu.VMEM)
    return pl.pallas_call(
        unpack_kernel,
        out_shape=(
            shape(16, FF), shape(16, NFFT), shape(48, D), shape(8, 16), shape(1, 16), shape(7, 16), shape(1, 48), shape(1, 40),
        ) + (shape(1, 16),) * 5,
        in_specs=[pl.BlockSpec(memory_space=pltpu.SMEM), whole],
        out_specs=(whole,) * 13,
        name="unpack",
    )(pos, t)


AXES = ("frame", "rec")


def index_of(z, yl, c, yh, x):
    return ((z * 2 + yl) * 2 + c) * 8 + yh * 4 + x


def groups_over(which):
    sizes = dict(z=8, yl=2, c=2, yh=2, x=4)
    kept = [n for n in sizes if n not in which]

    def walk(names, fixed):
        if not names:
            return [fixed]
        return [r for v in range(sizes[names[0]]) for r in walk(names[1:], {**fixed, names[0]: v})]

    return [[index_of(**g) for g in walk(list(which), fixed)] for fixed in walk(kept, {})]


def exchange(array, which):
    return lax.all_to_all(array, AXES, split_axis=0, concat_axis=0, axis_index_groups=groups_over(which), tiled=True)


def summed(array):
    return jnp.sum(array.astype(f32), axis=0)


def reduce_all(keep, send):
    pairs = groups_over(("c",))
    other = lax.ppermute(send, AXES, [(a, b) for a, b in pairs] + [(b, a) for a, b in pairs])
    half = (keep.astype(f32) + other.astype(f32)).astype(bf16).reshape(16, 8 * SUB, 128)
    part = summed(exchange(half, ("yl", "yh", "x"))).astype(bf16).reshape(8, SUB, 128)
    mine = summed(exchange(part, ("z",))).astype(bf16)
    return lax.all_to_all(jnp.broadcast_to(mine, (8, SUB, 128)), "rec", split_axis=0, concat_axis=0, tiled=True)


def body(code_indices, lengths, cotangent, *weights):
    count = lax.axis_size("frame")
    me = lax.axis_index("frame")
    codes = code_indices[0].T
    samples = cotangent[0].astype(f32).reshape(640, 128)
    low = samples.astype(bf16)
    codes_low = codes.astype(bf16)
    forward = [(i, i + 1) for i in range(count - 1)]
    backward = [(b, a) for a, b in forward]
    left = lax.ppermute(jnp.concatenate([low[640 - LEFT :], codes_low[:, FRAMES - 128 :]]), "frame", forward)
    right = lax.ppermute(jnp.concatenate([low[:LEFT], codes_low[:, :128]]), "frame", backward)
    pos = jnp.stack([me * FRAMES, lengths[0], count * FRAMES, me % 2]).astype(jnp.int32)
    flat = [w if w.ndim == 2 else w[None] if w.size == D else w.reshape(-1, 128) for w in weights]
    ready = setup([codes, *flat, jnp.asarray(edges())])
    t = reduce_all(*local_grads(pos, samples, left, right, ready))
    up_g, head_g, down_g, embed_w, embed_b, depth_k, up_b, head_b, *vectors = unpack(me.astype(jnp.int32)[None], t)
    depth_b, gain, bias, down_b, scale = (v[0] for v in vectors)
    return (
        embed_w, embed_b[0], depth_k, depth_b, gain, bias, up_g, up_b[0], down_g, down_b, scale, head_g, head_b[0],
    )


def solution(mesh):
    return jax.shard_map(
        body,
        mesh=mesh,
        in_specs=(P("rec", "frame", None), P("rec"), P("rec", "frame")) + (P(),) * 13,
        out_specs=(
            P(None, "frame"), P("frame"), P(None, "frame"), P("frame"), P("frame"), P("frame"), P("frame", None),
            P("frame"), P("frame", None), P("frame"), P("frame"), P("frame", None), P("frame"),
        ),
        check_vma=False,
    )
```

```python
import jax
import jax.numpy as jnp
import numpy as np
from jax import lax
from jax.experimental import pallas as pl
from jax.experimental.pallas import tpu as pltpu
from jax.sharding import PartitionSpec as P

D = 512
FF = 1536
Q = 8
KERNEL = 7
NFFT = 1280
HOP = 320
BINS = 640
PAD = 480
EPSILON = 1e-06
HALF = 3.5

FRAMES = 256
PAIRS = FRAMES // 2
ROWS = FRAMES + 16
LEFT = 24
SUB = 72
TAB = 1472
f32 = jnp.float32
bf16 = jnp.bfloat16


def tables():
    n = np.arange(16)[:, None]
    k = np.arange(BINS)[None, :]
    turn = 2.0 * np.pi / NFFT
    out = np.zeros((64, BINS), np.float64)
    out[0:16] = np.cos(turn * (n * k % NFFT))
    out[16:32] = np.sin(turn * (n * k % NFFT))
    out[32] = np.cos(turn * (16 * k[0] % NFFT))
    out[33] = np.sin(turn * (16 * k[0] % NFFT))
    out[34] = np.where(k[0] == 0, 1.0, 2.0) / NFFT
    out[35] = np.where(k[0] == 0, 0.0, -2.0) / NFFT
    out[36] = np.cos(turn * 16)
    out[37] = np.sin(turn * 16)
    out[40:56, 0:128] = np.cos(turn * n)
    out[40:56, 128:256] = np.sin(turn * n)
    return out.astype(np.float32)


def edges():
    def square(i):
        return np.where((i >= 0) & (i < NFFT), (0.5 - 0.5 * np.cos(2.0 * np.pi / NFFT * i)) ** 2, 0.0)

    s = np.arange(512)
    first = sum(square(s + PAD - HOP * t) for t in range(4))
    last = sum(square(s - 32 + HOP * t) for t in range(1, 5))
    out = np.zeros((8, 128), np.float64)
    out[0:4] = (1.0 / first).reshape(4, 128)
    out[4:8] = (1.0 / last).reshape(4, 128)
    return out.astype(np.float32)


def dot(a, b):
    return lax.dot_general(a, b, (((1,), (0,)), ((), ())), preferred_element_type=f32)


def dot_rows(a, b):
    return lax.dot_general(a, b, (((0,), (0,)), ((), ())), preferred_element_type=f32)


def dot_cols(a, b):
    return lax.dot_general(a, b, (((1,), (1,)), ((), ())), preferred_element_type=f32)


def sine_cosine(p):
    k = jnp.round(p * np.float32(2.0 / np.pi))
    r = p - k * np.float32(1.5703125)
    r = r - k * np.float32(4.837512969970703125e-4)
    r = r - k * np.float32(7.54978995489188216e-8)
    z = r * r
    s = r + r * z * (np.float32(-1.6666654611e-1) + z * (np.float32(8.3321608736e-3) + z * np.float32(-1.9515295891e-4)))
    c = 1.0 - 0.5 * z + z * z * (
        np.float32(4.166664568298827e-2) + z * (np.float32(-1.388731625493765e-3) + z * np.float32(2.443315711809948e-5))
    )
    q = k.astype(jnp.int32)
    odd = (q & 1) == 1
    sine = jnp.where(odd, c, s)
    cosine = jnp.where(odd, s, c)
    sine = jnp.where((q & 2) == 2, -sine, sine)
    cosine = jnp.where(((q + 1) & 2) == 2, -cosine, cosine)
    return sine, cosine


def split3(w):
    hi = w.astype(bf16)
    rest = w - hi.astype(f32)
    mid = rest.astype(bf16)
    low = (rest - mid.astype(f32)).astype(bf16)
    return hi, mid, low


def setup_kernel(*refs):
    count = (len(refs) - 4) // 2
    sources, trig_far, outs = refs[:count], refs[count], refs[count + 1 : -3]
    tab, trig, sems = refs[-3:]
    first = pltpu.make_async_copy(trig_far, trig, sems.at[count])
    copies = [pltpu.make_async_copy(a, b, sems.at[i]) for i, (a, b) in enumerate(zip(sources, outs))]
    first.start()
    for copy in copies:
        copy.start()

    tab[0:96, :] = jnp.zeros((96, NFFT), bf16)
    tab[1376:TAB, :] = jnp.zeros((TAB - 1376, NFFT), bf16)
    first.wait()
    cs, sn = trig[32:33, :], trig[33:34, :]
    real_row, imag_row = trig[34:35, :], trig[35:36, :]
    wcs, wsn = trig[36:37, 0:128], trig[37:38, 0:128]

    def table_step(i, carry):
        c, s, wc, ws = carry
        window = jnp.concatenate([0.5 - 0.5 * wc] * 5, axis=1)
        at = pl.multiple_of(96 + i * 16, 16)
        tab[pl.ds(at, 16), 0:BINS] = (c * (window * real_row)).astype(bf16)
        tab[pl.ds(at, 16), BINS:] = (s * (window * imag_row)).astype(bf16)
        return c * cs - s * sn, s * cs + c * sn, wc * wcs - ws * wsn, ws * wcs + wc * wsn

    lax.fori_loop(0, NFFT // 16, table_step, (trig[0:16, :], trig[16:32, :], trig[40:56, 0:128], trig[40:56, 128:256]))
    for copy in copies:
        copy.wait()


def setup(arrays):
    whole = pl.BlockSpec(memory_space=pltpu.VMEM)
    return pl.pallas_call(
        setup_kernel,
        out_shape=tuple(jax.ShapeDtypeStruct(a.shape, a.dtype) for a in arrays) + (jax.ShapeDtypeStruct((TAB, NFFT), bf16),),
        in_specs=[pl.BlockSpec(memory_space=pltpu.HBM)] * (len(arrays) + 1),
        out_specs=(whole,) * (len(arrays) + 1),
        scratch_shapes=[pltpu.VMEM((64, BINS), f32), pltpu.SemaphoreType.DMA((len(arrays) + 1,))],
        compiler_params=pltpu.CompilerParams(vmem_limit_bytes=16 * 1024 * 1024),
        name="setup",
    )(*[pltpu.with_memory_space_constraint(a, pltpu.HBM) for a in (*arrays, jnp.asarray(tables()))])


def local_kernel(
    pos, cot, left, right, codes, embed_w, embed_b, depth_k, depth_b, gain, bias, up_w, up_b, down_w, down_b,
    scale, head_w, head_b, edge, tab, keep, send,
    feat, conv, cgrad, latg, samp, pair_rows, spec_in, xhat, rstd, normed, hid, dgelu, act, branch, latent, re, im,
    logit_low, low, big, spec, lg, row_sums, sums, tiles, tall, rows,
):
    first_frame, length = pos[0], pos[1]
    last_frame = pos[2]
    core, my, mx = pos[3], pos[4], pos[5]

    def place(o, yl):
        part = o // SUB
        return (2 * (part // 4) + yl) ^ my, (part % 4) ^ mx

    for t in range(FF // 128):
        rows[0:1, 128 * t : 128 * t + 128] = up_b[t : t + 1, :]
    for t in range(NFFT // 128):
        rows[1:2, 128 * t : 128 * t + 128] = head_b[t : t + 1, :]
    up_row, head_row = rows[0:1, :], rows[1:2, 0:NFFT]

    w_hi, w_mid, w_low = split3(embed_w[...])

    def project(c):
        c = c.astype(bf16)
        return (dot_rows(c, w_hi) + dot_rows(c, w_mid) + dot_rows(c, w_low)) * np.float32(1.0 / HALF) + embed_b[...]

    own_codes = codes[...].astype(f32) - HALF
    feat[0:16, :] = jnp.zeros((16, D), f32)
    feat[16 + FRAMES :, :] = jnp.zeros((feat.shape[0] - 16 - FRAMES, D), f32)
    feat[16 : 16 + FRAMES, :] = project(own_codes)
    feat[8:16, :] = project(left[LEFT:, :].astype(f32) - HALF)[120:128, :]
    feat[16 + FRAMES : 24 + FRAMES, :] = project(right[LEFT:, :].astype(f32) - HALF)[0:8, :]

    def mask_step(i, _):
        at = pl.multiple_of(8 + i * 8, 8)
        frame = first_frame + (at - 16) + lax.broadcasted_iota(jnp.int32, (8, D), 0)
        keep = (frame >= 0) & (frame < length)
        feat[pl.ds(at, 8), :] = jnp.where(keep, feat[pl.ds(at, 8), :], 0.0).astype(bf16).astype(f32)
        return 0

    lax.fori_loop(0, (FRAMES + 16) // 8, mask_step, 0)

    taps = [depth_k[j : j + 1, :] for j in range(KERNEL)]
    total = jnp.broadcast_to(depth_b[...], (FRAMES + 16, D))
    for j in range(KERNEL):
        total = total + taps[j] * feat[5 + j : 5 + j + FRAMES + 16, :]
    conv[...] = total

    def to_rows(ref, base, dst):
        dst[0:FRAMES, :] = ref[base : base + FRAMES, :]
        dst[FRAMES : FRAMES + 8, :] = ref[base - 8 : base, :]
        dst[FRAMES + 8 :, :] = ref[base + FRAMES : base + FRAMES + 8, :]

    to_rows(conv, 8, xhat)

    x = xhat[...]
    centre = x - jnp.mean(x, axis=1, keepdims=True)
    r = lax.rsqrt(jnp.mean(centre * centre, axis=1, keepdims=True) + EPSILON)
    x = centre * r
    xhat[...] = x
    rstd[...] = jnp.broadcast_to(r, (ROWS, 128))
    normed[...] = (x * gain[...] + bias[...]).astype(bf16)

    hid[...] = dot(normed[...], up_w[...])

    def gelu_step(i, _):
        at = pl.ds(pl.multiple_of(i * 16, 16), 16)
        x = hid[at, :] + up_row
        cdf = 0.5 + 0.5 * lax.erf(x * np.float32(0.7071067811865476))
        act[at, :] = (x * cdf).astype(bf16)
        dgelu[at, :] = cdf + x * (jnp.exp(-0.5 * x * x) * np.float32(0.3989422804014327))
        return 0

    lax.fori_loop(0, ROWS // 16, gelu_step, 0)

    branch[...] = dot(act[...], down_w[...]) + down_b[...]
    to_rows(feat, 16, lg)
    latent[...] = (lg[...] + scale[...] * branch[...]).astype(bf16)

    big[0:ROWS, 0:NFFT] = dot(latent[...], head_w[...])

    def head_step(i, _):
        at = pl.ds(pl.multiple_of(i * 16, 16), 16)
        magnitude = jnp.exp(big[at, 0:BINS] + head_row[:, 0:BINS])
        sine, cosine = sine_cosine(big[at, BINS:NFFT] + head_row[:, BINS:])
        re[at, :] = magnitude * cosine
        im[at, :] = magnitude * sine
        return 0

    lax.fori_loop(0, ROWS // 16, head_step, 0)

    samp[0:LEFT, :] = left[0:LEFT, :].astype(f32)
    samp[LEFT : LEFT + 640, :] = cot[...]
    samp[LEFT + 640 :, :] = right[0:LEFT, :].astype(f32)
    start = first_frame * HOP
    limit = length * HOP

    def sample_step(i, _):
        at = pl.multiple_of(i * 8, 8)
        row = at - LEFT + lax.broadcasted_iota(jnp.int32, (8, 128), 0)
        s = start + row * 128 + lax.broadcasted_iota(jnp.int32, (8, 128), 1)
        x = samp[pl.ds(at, 8), :] * np.float32(2.0 / 3.0)
        samp[pl.ds(at, 8), :] = jnp.where(s < limit, x, 0.0)
        return 0

    def fix(at, values):
        row = at - LEFT + lax.broadcasted_iota(jnp.int32, (4, 128), 0)
        s = start + row * 128 + lax.broadcasted_iota(jnp.int32, (4, 128), 1)
        samp[at : at + 4, :] = jnp.where(s < limit, cot[at - LEFT : at - LEFT + 4, :] * values, 0.0)

    lax.fori_loop(0, (LEFT * 2 + 640) // 8, sample_step, 0)

    @pl.when(first_frame == 0)
    def _():
        fix(LEFT, edge[0:4, :])

    @pl.when(first_frame + FRAMES == last_frame)
    def _():
        fix(LEFT + 636, edge[4:8, :])

    for d in range(3):
        for k in range(5):
            column = (d * 5 + k) * 128
            base = LEFT + (d - 1) * 5 + k
            spec_in[0:PAIRS, column : column + 128] = samp[pl.ds(base, PAIRS, stride=5), :].astype(bf16)
            pair_rows[0:2, column : column + 128] = samp[pl.ds(base - 10, 2, stride=5), :]
            pair_rows[2:4, column : column + 128] = samp[pl.ds(base + 640, 2, stride=5), :]
    pair_rows[4:16, :] = jnp.zeros((12, 1920), f32)
    spec_in[PAIRS : PAIRS + 16, :] = pair_rows[...].astype(bf16)

    even = dot(spec_in[:, 128:1536], tab[64:1472, :])
    odd = dot(spec_in[:, 384:1792], tab[0:1408, :])
    for t in range(10):
        column = slice(128 * t, 128 * t + 128)
        spec[t, FRAMES:, :] = jnp.zeros((16, 128), f32)
        for part, parity in ((even, 0), (odd, 1)):
            spec[t, pl.ds(parity, PAIRS, stride=2), :] = part[0:PAIRS, column]
            spec[t, pl.ds(FRAMES + 4 + parity, 4, stride=2), :] = part[PAIRS : PAIRS + 4, column]

    def logit_grad_of(at):
        das, dps = [], []
        for t in range(5):
            column = slice(128 * t, 128 * t + 128)
            g_re, g_im = spec[t, at, :], spec[t + 5, at, :]
            r, m = re[at, column], im[at, column]
            da = g_re * r + g_im * m
            dp = g_im * r - g_re * m
            logit_low[at, column] = da.astype(bf16)
            logit_low[at, BINS + 128 * t : BINS + 128 * t + 128] = dp.astype(bf16)
            das.append(da)
            dps.append(dp)
        return jnp.concatenate(das, axis=1), jnp.concatenate(dps, axis=1)

    def logit_step(i, carry):
        da, dp = logit_grad_of(pl.ds(pl.multiple_of(i * 16, 16), 16))
        return carry[0] + da[0:8] + da[8:16], carry[1] + dp[0:8] + dp[8:16]

    zero = jnp.zeros((8, BINS), f32)
    da, dp = lax.fori_loop(0, FRAMES // 16, logit_step, (zero, zero))
    logit_grad_of(pl.ds(FRAMES, 16))
    head_sum = jnp.concatenate([jnp.sum(da, axis=0, keepdims=True), jnp.sum(dp, axis=0, keepdims=True)], axis=1)
    for t in range(10):
        tiles[16 + t : 17 + t, :] = head_sum[:, 128 * t : 128 * t + 128]

    latg[...] = dot_cols(logit_low[...], head_w[...])

    def scatter(big_ref, columns, height, row):
        def step(p, _):
            z, yl = p // 2, p % 2
            for ref, f in ((keep, 2 * p + core), (send, 2 * p + 1 - core)):
                for j in range(columns):
                    for h in range(height // 8):
                        o = row + j * height + h * 8
                        at = pl.multiple_of(f * height + h * 8, 8)
                        value = big_ref[pl.ds(at, 8), 128 * j : 128 * j + 128].astype(bf16)
                        dy, dx = place(o, yl)
                        ref[dy, dx, z, o % SUB : o % SUB + 8, :] = value
            return 0

        lax.fori_loop(0, 16, step, 0)

    big[0:D, 0:NFFT] = dot_rows(latent[0:FRAMES, :], logit_low[0:FRAMES, :])
    scatter(big, 10, 16, 192)

    def latent_step(i, carry):
        at = pl.ds(pl.multiple_of(i * 16, 16), 16)
        g = latg[at, :]
        low[at, :] = (scale[...] * g).astype(bf16)
        b = g * branch[at, :]
        return carry[0] + b[0:8] + b[8:16], carry[1] + g[0:8] + g[8:16]

    zero = jnp.zeros((8, D), f32)
    scale_sum, latent_sum = lax.fori_loop(0, FRAMES // 16, latent_step, (zero, zero))
    low[FRAMES:, :] = (scale[...] * latg[FRAMES:, :]).astype(bf16)
    sums[20:21, :] = jnp.sum(scale_sum, axis=0, keepdims=True)
    sums[19:20, :] = jnp.sum(latent_sum, axis=0, keepdims=True) * scale[...]

    tall[...] = dot_rows(act[0:FRAMES, :], low[0:FRAMES, :])
    scatter(tall, 4, 48, 352)

    hid[...] = dot_cols(low[...], down_w[...])

    def hidden_grad_of(at):
        g = hid[at, :] * dgelu[at, :]
        act[at, :] = g.astype(bf16)
        return g

    def hidden_step(i, carry):
        g = hidden_grad_of(pl.ds(pl.multiple_of(i * 16, 16), 16))
        return carry + g[0:8] + g[8:16]

    up_sum = lax.fori_loop(0, FRAMES // 16, hidden_step, jnp.zeros((8, FF), f32))
    hidden_grad_of(pl.ds(FRAMES, 16))
    up_sum = jnp.sum(up_sum, axis=0, keepdims=True)
    for t in range(12):
        tiles[t : t + 1, :] = up_sum[:, 128 * t : 128 * t + 128]

    big[0:D, 0:FF] = dot_rows(normed[0:FRAMES, :], act[0:FRAMES, :])
    scatter(big, 12, 16, 0)

    lg[...] = dot_cols(act[...], up_w[...])

    g, x = lg[...], xhat[...]
    dx = g * gain[...]
    m1 = jnp.mean(dx, axis=1, keepdims=True)
    m2 = jnp.mean(dx * x, axis=1, keepdims=True)
    lg[...] = rstd[:, 0:1] * (dx - m1 - x * m2)
    sums[17:18, :] = jnp.sum(g[0:FRAMES] * x[0:FRAMES], axis=0, keepdims=True)
    sums[18:19, :] = jnp.sum(g[0:FRAMES], axis=0, keepdims=True)

    i = lax.broadcasted_iota(jnp.int32, (16, D), 0)
    frame = jnp.where(i < 8, i - 8, i + (FRAMES - 8)) + first_frame
    inside = (frame >= 0) & (frame < last_frame)
    edge_rows = jnp.where(inside, lg[FRAMES:, :], 0.0)

    cgrad[0:8, :] = edge_rows[0:8]
    cgrad[8 : 8 + FRAMES, :] = lg[0:FRAMES, :]
    cgrad[8 + FRAMES :, :] = edge_rows[8:16]

    own = cgrad[8 : 8 + FRAMES, :]
    sums[16:17, :] = jnp.sum(own, axis=0, keepdims=True)
    total = latg[0:FRAMES, :]
    for j in range(KERNEL):
        sums[9 + j : 10 + j, :] = jnp.sum(own * feat[13 + j : 13 + j + FRAMES, :], axis=0, keepdims=True)
        total = total + taps[j] * cgrad[11 - j : 11 - j + FRAMES, :]
    frame = first_frame + lax.broadcasted_iota(jnp.int32, (FRAMES, D), 0)
    total = jnp.where(frame < length, total, 0.0)
    sums[8:9, :] = jnp.sum(total, axis=0, keepdims=True)
    hi, mid, rest = split3(total)
    own_low = own_codes.astype(bf16)
    sums[0:8, :] = (dot(own_low, hi) + dot(own_low, mid) + dot(own_low, rest)) * np.float32(1.0 / HALF)
    sums[21:24, :] = jnp.zeros((3, D), f32)

    tiles[12:16, :] = jnp.zeros((4, 128), f32)
    tiles[26:32, :] = jnp.zeros((6, 128), f32)
    row_sums[...] = jnp.zeros((8, 128), f32)

    def small_step(p, _):
        z, yl = p // 2, p % 2
        for ref, f in ((keep, 2 * p + core), (send, 2 * p + 1 - core)):
            row_sums[0:2, :] = tiles[pl.ds((48 * f) // 128, 2), :]
            row_sums[2:4, :] = tiles[pl.ds(16 + (40 * f) // 128, 2), :]
            dy, dx = place(7 * SUB, yl)
            ref[dy, dx, z, 64:72, :] = row_sums[...].astype(bf16)
        return 0

    lax.fori_loop(0, 16, small_step, 0)
    for p in range(16):
        column = 128 * (p // 4)
        part = sums[:, column : column + 128].astype(bf16)
        dy, dx = place(7 * SUB, p % 2)
        keep[dy, dx, p // 2, 40:64, :] = part
        send[dy, dx, p // 2, 40:64, :] = part


def local_grads(pos, cot, left, right, ready):
    vmem = pltpu.VMEM
    scratch = [
        vmem((FRAMES + 32, D), f32),
        vmem((FRAMES + 16, D), f32),
        vmem((FRAMES + 16, D), f32),
        vmem((ROWS, D), f32),
        vmem((640 + 2 * LEFT, 128), f32),
        vmem((16, 1920), f32),
        vmem((PAIRS + 16, 1920), bf16),
        vmem((ROWS, D), f32),
        vmem((ROWS, 128), f32),
        vmem((ROWS, D), bf16),
        vmem((ROWS, FF), f32),
        vmem((ROWS, FF), f32),
        vmem((ROWS, FF), bf16),
        vmem((ROWS, D), f32),
        vmem((ROWS, D), bf16),
        vmem((ROWS, BINS), f32),
        vmem((ROWS, BINS), f32),
        vmem((ROWS, NFFT), bf16),
        vmem((ROWS, D), bf16),
        vmem((D, FF), f32),
        vmem((10, ROWS, 128), f32),
        vmem((ROWS, D), f32),
        vmem((8, 128), f32),
        vmem((24, D), f32),
        vmem((32, 128), f32),
        vmem((FF, D), f32),
        vmem((8, FF), f32),
    ]
    whole = pl.BlockSpec(memory_space=pltpu.VMEM)
    arrays = [cot, left, right, *ready]
    return pl.pallas_call(
        local_kernel,
        out_shape=(jax.ShapeDtypeStruct((4, 4, 8, SUB, 128), bf16),) * 2,
        in_specs=[pl.BlockSpec(memory_space=pltpu.SMEM)] + [whole] * len(arrays),
        out_specs=(whole, whole),
        scratch_shapes=scratch,
        compiler_params=pltpu.CompilerParams(vmem_limit_bytes=38 * 1024 * 1024),
        name="local_grads",
    )(pos, *arrays)


def unpack_kernel(pos, t, up_g, head_g, down_g, embed_w, embed_b, depth_k, up_b, head_b, *vectors):
    f = pos[0]

    def tile(o):
        return t[o // SUB, o % SUB : o % SUB + 8, :].astype(f32)

    for columns, height, row, ref in ((12, 16, 0, up_g), (10, 16, 192, head_g), (4, 48, 352, down_g)):
        for j in range(columns):
            for h in range(height // 8):
                ref[h * 8 : h * 8 + 8, 128 * j : 128 * j + 128] = tile(row + j * height + h * 8)
    shift = 16 * (f % 8)
    back = lax.rem(128 - shift, 128)

    def rolled(x, by):
        return pltpu.roll(x, by, 1)

    embed_w[...] = rolled(tile(544), back)[:, 0:16]
    second = rolled(tile(552), back)
    third = rolled(tile(560), back)
    embed_b[...] = second[0:1, 0:16]
    depth_k[...] = second[1:8, 0:16]
    for i, ref in enumerate(vectors):
        ref[...] = third[i : i + 1, 0:16]
    last = tile(568)
    lane = lax.broadcasted_iota(jnp.int32, (1, 128), 1)
    for row, width, ref in ((0, 48, up_b), (2, 40, head_b)):
        shift = lax.rem(width * f, 128)
        back = lax.rem(128 - shift, 128)
        moved = rolled(last, back)
        joined = jnp.where(lane < 128 - shift, moved[row : row + 1, :], moved[row + 1 : row + 2, :])
        ref[...] = joined[:, 0:width]


def unpack(pos, t):
    def shape(*s):
        return jax.ShapeDtypeStruct(s, f32)

    whole = pl.BlockSpec(memory_space=pltpu.VMEM)
    return pl.pallas_call(
        unpack_kernel,
        out_shape=(
            shape(16, FF), shape(16, NFFT), shape(48, D), shape(8, 16), shape(1, 16), shape(7, 16), shape(1, 48), shape(1, 40),
        ) + (shape(1, 16),) * 5,
        in_specs=[pl.BlockSpec(memory_space=pltpu.SMEM), whole],
        out_specs=(whole,) * 13,
        name="unpack",
    )(pos, t)


AXES = ("frame", "rec")


def index_of(z, yl, c, yh, x):
    return ((z * 2 + yl) * 2 + c) * 8 + yh * 4 + x


def groups_over(which):
    sizes = dict(z=8, yl=2, c=2, yh=2, x=4)
    kept = [n for n in sizes if n not in which]

    def walk(names, fixed):
        if not names:
            return [fixed]
        return [r for v in range(sizes[names[0]]) for r in walk(names[1:], {**fixed, names[0]: v})]

    return [[index_of(**g) for g in walk(list(which), fixed)] for fixed in walk(kept, {})]


def exchange(array, which):
    return lax.all_to_all(array, AXES, split_axis=0, concat_axis=0, axis_index_groups=groups_over(which), tiled=True)


def summed(array):
    return jnp.sum(array.astype(f32), axis=0)


def partners(which, offset=0):
    pairs = []
    for z in range(8):
        for y in range(4):
            for c in range(2):
                for x in range(4):
                    flip = 3 if offset else 1
                    to = dict(c=(y, 1 - c, x), x=(y, c, x ^ flip), y=(y ^ flip, c, x))[which]
                    pairs.append((index_of(z, y % 2, c, y // 2, x), index_of(z, to[0] % 2, to[1], to[0] // 2, to[2])))
    return pairs


ORDERS = ((0, 3, 1, 2), (0, 1, 3, 2))
AXIS_OF = ("x", "x", "y", "y")


def split_first(keep, other, *outs):
    for k in range(4):
        for i, d in enumerate(ORDERS[k % 2]):
            for e in range(4):
                for z in range(2):
                    at = ((e, d) if k < 2 else (d, e)) + (2 * k + z,)
                    total = keep[at].astype(f32) + other[at].astype(f32)
                    if i < 2:
                        outs[4 + k][i, e, z] = total
                    else:
                        outs[k][i - 2, e, z] = total.astype(bf16)


def split_second(*refs):
    keeps, others, outs = refs[0:4], refs[4:8], refs[8:]
    for k in range(4):
        for e in range(4):
            for z in range(2):
                outs[4 + k][e, z] = keeps[k][0, e, z] + others[k][0, e, z].astype(f32)
                outs[k][e, z] = (keeps[k][1, e, z] + others[k][1, e, z].astype(f32)).astype(bf16)


def split_third(*refs):
    keeps, others, outs = refs[0:4], refs[4:8], refs[8:]
    for g in range(2):
        for h in range(2):
            k = 2 * g + h
            for i, d in enumerate(ORDERS[0]):
                for z in range(2):
                    total = keeps[k][d, z] + others[k][d, z].astype(f32)
                    if i < 2:
                        outs[2 + g][i, 2 * h + z] = total
                    else:
                        outs[g][i - 2, 2 * h + z] = total.astype(bf16)


def split_fourth(*refs):
    keeps, others, outs = refs[0:2], refs[2:4], refs[4:]
    for g in range(2):
        for z in range(4):
            outs[2 + g][z] = keeps[g][0, z] + others[g][0, z].astype(f32)
            outs[g][z] = (keeps[g][1, z] + others[g][1, z].astype(f32)).astype(bf16)


def join(*refs):
    for g in range(2):
        for z in range(4):
            refs[4][4 * g + z] = (refs[g][z] + refs[2 + g][z].astype(f32)).astype(bf16)


def step(kernel, arrays, shape, count, limit):
    whole = pl.BlockSpec(memory_space=pltpu.VMEM)
    kinds = (bf16,) * count + (f32,) * (count if kernel is not join else 0)
    return pl.pallas_call(
        kernel,
        out_shape=tuple(jax.ShapeDtypeStruct(shape + (SUB, 128), kind) for kind in kinds),
        in_specs=[whole] * len(arrays),
        out_specs=(whole,) * len(kinds),
        compiler_params=pltpu.CompilerParams(vmem_limit_bytes=limit * 1024 * 1024),
        name=kernel.__name__,
    )(*arrays)


def reduce_all(keep, send):
    other = lax.ppermute(send, AXES, partners("c"))
    parts = step(split_first, (keep, other), (2, 4, 2), 4, 24)
    moved = [lax.ppermute(a, AXES, partners(AXIS_OF[k], k % 2)) for k, a in enumerate(parts[:4])]
    parts = step(split_second, (*parts[4:], *moved), (4, 2), 4, 16)
    moved = [lax.ppermute(a, AXES, partners(AXIS_OF[k], 1 - k % 2)) for k, a in enumerate(parts[:4])]
    parts = step(split_third, (*parts[4:], *moved), (2, 4), 2, 8)
    moved = [lax.ppermute(a, AXES, partners("yx"[g], 0)) for g, a in enumerate(parts[:2])]
    parts = step(split_fourth, (*parts[2:], *moved), (4,), 2, 8)
    moved = [lax.ppermute(a, AXES, partners("yx"[g], 1)) for g, a in enumerate(parts[:2])]
    (part,) = step(join, (*parts[2:], *moved), (8,), 1, 8)
    mine = summed(exchange(part, ("z",))).astype(bf16)
    return lax.all_to_all(jnp.broadcast_to(mine, (8, SUB, 128)), "rec", split_axis=0, concat_axis=0, tiled=True)


def body(code_indices, lengths, cotangent, *weights):
    count = lax.axis_size("frame")
    me, rec = lax.axis_index("frame"), lax.axis_index("rec")
    codes = code_indices[0].T
    samples = cotangent[0].astype(f32).reshape(640, 128)
    low = samples.astype(bf16)
    codes_low = codes.astype(bf16)
    forward = [(i, i + 1) for i in range(count - 1)]
    backward = [(b, a) for a, b in forward]
    left = lax.ppermute(jnp.concatenate([low[640 - LEFT :], codes_low[:, FRAMES - 128 :]]), "frame", forward)
    right = lax.ppermute(jnp.concatenate([low[:LEFT], codes_low[:, :128]]), "frame", backward)
    pos = jnp.stack([me * FRAMES, lengths[0], count * FRAMES, me % 2, 2 * (rec // 4) + me // 2 % 2, rec % 4]).astype(jnp.int32)
    flat = [w if w.ndim == 2 else w[None] if w.size == D else w.reshape(-1, 128) for w in weights]
    ready = setup([codes, *flat, jnp.asarray(edges())])
    t = reduce_all(*local_grads(pos, samples, left, right, ready))
    up_g, head_g, down_g, embed_w, embed_b, depth_k, up_b, head_b, *vectors = unpack(me.astype(jnp.int32)[None], t)
    depth_b, gain, bias, down_b, scale = (v[0] for v in vectors)
    return (
        embed_w, embed_b[0], depth_k, depth_b, gain, bias, up_g, up_b[0], down_g, down_b, scale, head_g, head_b[0],
    )


def solution(mesh):
    return jax.shard_map(
        body,
        mesh=mesh,
        in_specs=(P("rec", "frame", None), P("rec"), P("rec", "frame")) + (P(),) * 13,
        out_specs=(
            P(None, "frame"), P("frame"), P(None, "frame"), P("frame"), P("frame"), P("frame"), P("frame", None),
            P("frame"), P("frame", None), P("frame"), P("frame"), P("frame", None), P("frame"),
        ),
        check_vma=False,
    )
```

```python
import jax
import jax.numpy as jnp
import numpy as np
from jax import lax
from jax.experimental import pallas as pl
from jax.experimental.pallas import tpu as pltpu
from jax.sharding import PartitionSpec as P

D = 512
FF = 1536
Q = 8
KERNEL = 7
NFFT = 1280
HOP = 320
BINS = 640
PAD = 480
EPSILON = 1e-06
HALF = 3.5

FRAMES = 256
PAIRS = FRAMES // 2
ROWS = FRAMES + 16
LEFT = 24
SUB = 72
TAB = 1472
f32 = jnp.float32
bf16 = jnp.bfloat16


def tables():
    n = np.arange(16)[:, None]
    k = np.arange(BINS)[None, :]
    turn = 2.0 * np.pi / NFFT
    out = np.zeros((64, BINS), np.float64)
    out[0:16] = np.cos(turn * (n * k % NFFT))
    out[16:32] = np.sin(turn * (n * k % NFFT))
    out[32] = np.cos(turn * (16 * k[0] % NFFT))
    out[33] = np.sin(turn * (16 * k[0] % NFFT))
    out[34] = np.where(k[0] == 0, 1.0, 2.0) / NFFT
    out[35] = np.where(k[0] == 0, 0.0, -2.0) / NFFT
    out[36] = np.cos(turn * 16)
    out[37] = np.sin(turn * 16)
    out[40:56, 0:128] = np.cos(turn * n)
    out[40:56, 128:256] = np.sin(turn * n)
    return out.astype(np.float32)


def edges():
    def square(i):
        return np.where((i >= 0) & (i < NFFT), (0.5 - 0.5 * np.cos(2.0 * np.pi / NFFT * i)) ** 2, 0.0)

    s = np.arange(512)
    first = sum(square(s + PAD - HOP * t) for t in range(4))
    last = sum(square(s - 32 + HOP * t) for t in range(1, 5))
    out = np.zeros((8, 128), np.float64)
    out[0:4] = (1.0 / first).reshape(4, 128)
    out[4:8] = (1.0 / last).reshape(4, 128)
    return out.astype(np.float32)


def dot(a, b):
    return lax.dot_general(a, b, (((1,), (0,)), ((), ())), preferred_element_type=f32)


def dot_rows(a, b):
    return lax.dot_general(a, b, (((0,), (0,)), ((), ())), preferred_element_type=f32)


def dot_cols(a, b):
    return lax.dot_general(a, b, (((1,), (1,)), ((), ())), preferred_element_type=f32)


def sine_cosine(p):
    k = jnp.round(p * np.float32(2.0 / np.pi))
    r = p - k * np.float32(1.5703125)
    r = r - k * np.float32(4.837512969970703125e-4)
    r = r - k * np.float32(7.54978995489188216e-8)
    z = r * r
    s = r + r * z * (np.float32(-1.6666654611e-1) + z * (np.float32(8.3321608736e-3) + z * np.float32(-1.9515295891e-4)))
    c = 1.0 - 0.5 * z + z * z * (
        np.float32(4.166664568298827e-2) + z * (np.float32(-1.388731625493765e-3) + z * np.float32(2.443315711809948e-5))
    )
    q = k.astype(jnp.int32)
    odd = (q & 1) == 1
    sine = jnp.where(odd, c, s)
    cosine = jnp.where(odd, s, c)
    sine = jnp.where((q & 2) == 2, -sine, sine)
    cosine = jnp.where(((q + 1) & 2) == 2, -cosine, cosine)
    return sine, cosine


def split3(w):
    hi = w.astype(bf16)
    rest = w - hi.astype(f32)
    mid = rest.astype(bf16)
    low = (rest - mid.astype(f32)).astype(bf16)
    return hi, mid, low


def setup_kernel(*refs):
    count = (len(refs) - 4) // 2
    sources, trig_far, outs = refs[:count], refs[count], refs[count + 1 : -3]
    tab, trig, sems = refs[-3:]
    first = pltpu.make_async_copy(trig_far, trig, sems.at[count])
    copies = [pltpu.make_async_copy(a, b, sems.at[i]) for i, (a, b) in enumerate(zip(sources, outs))]
    first.start()
    for copy in copies:
        copy.start()

    tab[0:96, :] = jnp.zeros((96, NFFT), bf16)
    tab[1376:TAB, :] = jnp.zeros((TAB - 1376, NFFT), bf16)
    first.wait()
    cs, sn = trig[32:33, :], trig[33:34, :]
    real_row, imag_row = trig[34:35, :], trig[35:36, :]
    wcs, wsn = trig[36:37, 0:128], trig[37:38, 0:128]

    def table_step(i, carry):
        c, s, wc, ws = carry
        window = jnp.concatenate([0.5 - 0.5 * wc] * 5, axis=1)
        at = pl.multiple_of(96 + i * 16, 16)
        tab[pl.ds(at, 16), 0:BINS] = (c * (window * real_row)).astype(bf16)
        tab[pl.ds(at, 16), BINS:] = (s * (window * imag_row)).astype(bf16)
        return c * cs - s * sn, s * cs + c * sn, wc * wcs - ws * wsn, ws * wcs + wc * wsn

    lax.fori_loop(0, NFFT // 16, table_step, (trig[0:16, :], trig[16:32, :], trig[40:56, 0:128], trig[40:56, 128:256]))
    for copy in copies:
        copy.wait()


def setup(arrays):
    whole = pl.BlockSpec(memory_space=pltpu.VMEM)
    return pl.pallas_call(
        setup_kernel,
        out_shape=tuple(jax.ShapeDtypeStruct(a.shape, a.dtype) for a in arrays) + (jax.ShapeDtypeStruct((TAB, NFFT), bf16),),
        in_specs=[pl.BlockSpec(memory_space=pltpu.HBM)] * (len(arrays) + 1),
        out_specs=(whole,) * (len(arrays) + 1),
        scratch_shapes=[pltpu.VMEM((64, BINS), f32), pltpu.SemaphoreType.DMA((len(arrays) + 1,))],
        compiler_params=pltpu.CompilerParams(vmem_limit_bytes=16 * 1024 * 1024),
        name="setup",
    )(*[pltpu.with_memory_space_constraint(a, pltpu.HBM) for a in (*arrays, jnp.asarray(tables()))])


def local_kernel(
    pos, cot, left, right, codes, embed_w, embed_b, depth_k, depth_b, gain, bias, up_w, up_b, down_w, down_b,
    scale, head_w, head_b, edge, tab, keep, send,
    feat, conv, cgrad, latg, samp, pair_rows, spec_in, xhat, rstd, normed, hid, dgelu, act, branch, latent, re, im,
    logit_low, low, big, spec, lg, sums, tiles, tall, rows,
):
    me, rec = lax.axis_index("frame"), lax.axis_index("rec")
    first_frame, length = me * FRAMES, pos[0]
    last_frame = lax.axis_size("frame") * FRAMES
    core, my, mx = me & 1, 2 * (rec >> 2) + ((me >> 1) & 1), rec & 3

    def place(o, yl):
        part = o // SUB
        return (2 * (part // 4) + yl) ^ my, (part % 4) ^ mx

    for t in range(FF // 128):
        rows[0:1, 128 * t : 128 * t + 128] = up_b[t : t + 1, :]
    for t in range(NFFT // 128):
        rows[1:2, 128 * t : 128 * t + 128] = head_b[t : t + 1, :]
    up_row, head_row = rows[0:1, :], rows[1:2, 0:NFFT]

    w_hi, w_mid, w_low = split3(embed_w[...])

    def project(c):
        c = c.astype(bf16)
        return (dot_rows(c, w_hi) + dot_rows(c, w_mid) + dot_rows(c, w_low)) * np.float32(1.0 / HALF) + embed_b[...]

    own_codes = codes[...].astype(f32) - HALF
    feat[0:16, :] = jnp.zeros((16, D), f32)
    feat[16 + FRAMES :, :] = jnp.zeros((feat.shape[0] - 16 - FRAMES, D), f32)
    feat[16 : 16 + FRAMES, :] = project(own_codes)
    feat[8:16, :] = project(left[LEFT:, :].astype(f32) - HALF)[120:128, :]
    feat[16 + FRAMES : 24 + FRAMES, :] = project(right[LEFT:, :].astype(f32) - HALF)[0:8, :]

    def mask_step(i, _):
        at = pl.multiple_of(8 + i * 8, 8)
        frame = first_frame + (at - 16) + lax.broadcasted_iota(jnp.int32, (8, D), 0)
        keep = (frame >= 0) & (frame < length)
        feat[pl.ds(at, 8), :] = jnp.where(keep, feat[pl.ds(at, 8), :], 0.0).astype(bf16).astype(f32)
        return 0

    lax.fori_loop(0, (FRAMES + 16) // 8, mask_step, 0)

    taps = [depth_k[j : j + 1, :] for j in range(KERNEL)]
    total = jnp.broadcast_to(depth_b[...], (FRAMES + 16, D))
    for j in range(KERNEL):
        total = total + taps[j] * feat[5 + j : 5 + j + FRAMES + 16, :]
    conv[...] = total

    def to_rows(ref, base, dst):
        dst[0:FRAMES, :] = ref[base : base + FRAMES, :]
        dst[FRAMES : FRAMES + 8, :] = ref[base - 8 : base, :]
        dst[FRAMES + 8 :, :] = ref[base + FRAMES : base + FRAMES + 8, :]

    to_rows(conv, 8, xhat)

    x = xhat[...]
    centre = x - jnp.mean(x, axis=1, keepdims=True)
    r = lax.rsqrt(jnp.mean(centre * centre, axis=1, keepdims=True) + EPSILON)
    x = centre * r
    xhat[...] = x
    rstd[...] = jnp.broadcast_to(r, (ROWS, 128))
    normed[...] = (x * gain[...] + bias[...]).astype(bf16)

    hid[...] = dot(normed[...], up_w[...])

    def gelu_step(i, _):
        at = pl.ds(pl.multiple_of(i * 16, 16), 16)
        x = hid[at, :] + up_row
        cdf = 0.5 + 0.5 * lax.erf(x * np.float32(0.7071067811865476))
        act[at, :] = (x * cdf).astype(bf16)
        dgelu[at, :] = cdf + x * (jnp.exp(-0.5 * x * x) * np.float32(0.3989422804014327))
        return 0

    lax.fori_loop(0, ROWS // 16, gelu_step, 0)

    branch[...] = dot(act[...], down_w[...]) + down_b[...]
    to_rows(feat, 16, lg)
    latent[...] = (lg[...] + scale[...] * branch[...]).astype(bf16)

    big[0:ROWS, 0:NFFT] = dot(latent[...], head_w[...])

    def head_step(i, _):
        at = pl.ds(pl.multiple_of(i * 16, 16), 16)
        magnitude = jnp.exp(big[at, 0:BINS] + head_row[:, 0:BINS])
        sine, cosine = sine_cosine(big[at, BINS:NFFT] + head_row[:, BINS:])
        re[at, :] = magnitude * cosine
        im[at, :] = magnitude * sine
        return 0

    lax.fori_loop(0, ROWS // 16, head_step, 0)

    samp[0:LEFT, :] = left[0:LEFT, :].astype(f32)
    samp[LEFT : LEFT + 640, :] = cot[...]
    samp[LEFT + 640 :, :] = right[0:LEFT, :].astype(f32)
    start = first_frame * HOP
    limit = length * HOP

    def sample_step(i, _):
        at = pl.multiple_of(i * 8, 8)
        row = at - LEFT + lax.broadcasted_iota(jnp.int32, (8, 128), 0)
        s = start + row * 128 + lax.broadcasted_iota(jnp.int32, (8, 128), 1)
        x = samp[pl.ds(at, 8), :] * np.float32(2.0 / 3.0)
        samp[pl.ds(at, 8), :] = jnp.where(s < limit, x, 0.0)
        return 0

    def fix(at, values):
        row = at - LEFT + lax.broadcasted_iota(jnp.int32, (4, 128), 0)
        s = start + row * 128 + lax.broadcasted_iota(jnp.int32, (4, 128), 1)
        samp[at : at + 4, :] = jnp.where(s < limit, cot[at - LEFT : at - LEFT + 4, :] * values, 0.0)

    lax.fori_loop(0, (LEFT * 2 + 640) // 8, sample_step, 0)

    @pl.when(first_frame == 0)
    def _():
        fix(LEFT, edge[0:4, :])

    @pl.when(first_frame + FRAMES == last_frame)
    def _():
        fix(LEFT + 636, edge[4:8, :])

    for d in range(3):
        for k in range(5):
            column = (d * 5 + k) * 128
            base = LEFT + (d - 1) * 5 + k
            spec_in[0:PAIRS, column : column + 128] = samp[pl.ds(base, PAIRS, stride=5), :].astype(bf16)
            pair_rows[0:2, column : column + 128] = samp[pl.ds(base - 10, 2, stride=5), :]
            pair_rows[2:4, column : column + 128] = samp[pl.ds(base + 640, 2, stride=5), :]
    pair_rows[4:16, :] = jnp.zeros((12, 1920), f32)
    spec_in[PAIRS : PAIRS + 16, :] = pair_rows[...].astype(bf16)

    even = dot(spec_in[:, 128:1536], tab[64:1472, :])
    odd = dot(spec_in[:, 384:1792], tab[0:1408, :])
    for t in range(10):
        column = slice(128 * t, 128 * t + 128)
        spec[t, FRAMES:, :] = jnp.zeros((16, 128), f32)
        for part, parity in ((even, 0), (odd, 1)):
            spec[t, pl.ds(parity, PAIRS, stride=2), :] = part[0:PAIRS, column]
            spec[t, pl.ds(FRAMES + 4 + parity, 4, stride=2), :] = part[PAIRS : PAIRS + 4, column]

    def logit_grad_of(at):
        das, dps = [], []
        for t in range(5):
            column = slice(128 * t, 128 * t + 128)
            g_re, g_im = spec[t, at, :], spec[t + 5, at, :]
            r, m = re[at, column], im[at, column]
            da = g_re * r + g_im * m
            dp = g_im * r - g_re * m
            logit_low[at, column] = da.astype(bf16)
            logit_low[at, BINS + 128 * t : BINS + 128 * t + 128] = dp.astype(bf16)
            das.append(da)
            dps.append(dp)
        return jnp.concatenate(das, axis=1), jnp.concatenate(dps, axis=1)

    def logit_step(i, carry):
        da, dp = logit_grad_of(pl.ds(pl.multiple_of(i * 16, 16), 16))
        return carry[0] + da[0:8] + da[8:16], carry[1] + dp[0:8] + dp[8:16]

    zero = jnp.zeros((8, BINS), f32)
    da, dp = lax.fori_loop(0, FRAMES // 16, logit_step, (zero, zero))
    logit_grad_of(pl.ds(FRAMES, 16))
    head_sum = jnp.concatenate([jnp.sum(da, axis=0, keepdims=True), jnp.sum(dp, axis=0, keepdims=True)], axis=1)
    for t in range(10):
        tiles[16 + t : 17 + t, :] = head_sum[:, 128 * t : 128 * t + 128]

    latg[...] = dot_cols(logit_low[...], head_w[...])

    def scatter(big_ref, columns, height, row):
        def step(p, _):
            z, yl = p // 2, p % 2
            for ref, f in ((keep, 2 * p + core), (send, 2 * p + 1 - core)):
                for j in range(columns):
                    for h in range(height // 8):
                        o = row + j * height + h * 8
                        at = pl.multiple_of(f * height + h * 8, 8)
                        value = big_ref[pl.ds(at, 8), 128 * j : 128 * j + 128].astype(bf16)
                        dy, dx = place(o, yl)
                        ref[dy, dx, z, o % SUB : o % SUB + 8, :] = value
            return 0

        lax.fori_loop(0, 16, step, 0)

    big[0:D, 0:NFFT] = dot_rows(latent[0:FRAMES, :], logit_low[0:FRAMES, :])
    scatter(big, 10, 16, 192)

    def latent_step(i, carry):
        at = pl.ds(pl.multiple_of(i * 16, 16), 16)
        g = latg[at, :]
        low[at, :] = (scale[...] * g).astype(bf16)
        b = g * branch[at, :]
        return carry[0] + b[0:8] + b[8:16], carry[1] + g[0:8] + g[8:16]

    zero = jnp.zeros((8, D), f32)
    scale_sum, latent_sum = lax.fori_loop(0, FRAMES // 16, latent_step, (zero, zero))
    low[FRAMES:, :] = (scale[...] * latg[FRAMES:, :]).astype(bf16)
    sums[20:21, :] = jnp.sum(scale_sum, axis=0, keepdims=True)
    sums[19:20, :] = jnp.sum(latent_sum, axis=0, keepdims=True) * scale[...]

    tall[...] = dot_rows(act[0:FRAMES, :], low[0:FRAMES, :])
    scatter(tall, 4, 48, 352)

    hid[...] = dot_cols(low[...], down_w[...])

    def hidden_grad_of(at):
        g = hid[at, :] * dgelu[at, :]
        act[at, :] = g.astype(bf16)
        return g

    def hidden_step(i, carry):
        g = hidden_grad_of(pl.ds(pl.multiple_of(i * 16, 16), 16))
        return carry + g[0:8] + g[8:16]

    up_sum = lax.fori_loop(0, FRAMES // 16, hidden_step, jnp.zeros((8, FF), f32))
    hidden_grad_of(pl.ds(FRAMES, 16))
    up_sum = jnp.sum(up_sum, axis=0, keepdims=True)
    for t in range(12):
        tiles[t : t + 1, :] = up_sum[:, 128 * t : 128 * t + 128]

    big[0:D, 0:FF] = dot_rows(normed[0:FRAMES, :], act[0:FRAMES, :])
    scatter(big, 12, 16, 0)

    lg[...] = dot_cols(act[...], up_w[...])

    g, x = lg[...], xhat[...]
    dx = g * gain[...]
    m1 = jnp.mean(dx, axis=1, keepdims=True)
    m2 = jnp.mean(dx * x, axis=1, keepdims=True)
    lg[...] = rstd[:, 0:1] * (dx - m1 - x * m2)
    sums[17:18, :] = jnp.sum(g[0:FRAMES] * x[0:FRAMES], axis=0, keepdims=True)
    sums[18:19, :] = jnp.sum(g[0:FRAMES], axis=0, keepdims=True)

    i = lax.broadcasted_iota(jnp.int32, (16, D), 0)
    frame = jnp.where(i < 8, i - 8, i + (FRAMES - 8)) + first_frame
    inside = (frame >= 0) & (frame < last_frame)
    edge_rows = jnp.where(inside, lg[FRAMES:, :], 0.0)

    cgrad[0:8, :] = edge_rows[0:8]
    cgrad[8 : 8 + FRAMES, :] = lg[0:FRAMES, :]
    cgrad[8 + FRAMES :, :] = edge_rows[8:16]

    own = cgrad[8 : 8 + FRAMES, :]
    sums[16:17, :] = jnp.sum(own, axis=0, keepdims=True)
    total = latg[0:FRAMES, :]
    for j in range(KERNEL):
        sums[9 + j : 10 + j, :] = jnp.sum(own * feat[13 + j : 13 + j + FRAMES, :], axis=0, keepdims=True)
        total = total + taps[j] * cgrad[11 - j : 11 - j + FRAMES, :]
    frame = first_frame + lax.broadcasted_iota(jnp.int32, (FRAMES, D), 0)
    total = jnp.where(frame < length, total, 0.0)
    sums[8:9, :] = jnp.sum(total, axis=0, keepdims=True)
    hi, mid, rest = split3(total)
    own_low = own_codes.astype(bf16)
    sums[0:8, :] = (dot(own_low, hi) + dot(own_low, mid) + dot(own_low, rest)) * np.float32(1.0 / HALF)
    sums[21:24, :] = jnp.zeros((3, D), f32)

    tiles[12:16, :] = jnp.zeros((4, 128), f32)
    tiles[26:32, :] = jnp.zeros((6, 128), f32)
    blank = jnp.zeros((4, 128), f32)

    def bias_rows(f):
        up, head = 48 * f // 128, 16 + 40 * f // 128
        return jnp.concatenate([tiles[up : up + 2, :], tiles[head : head + 2, :], blank], axis=0).astype(bf16)

    for p in range(16):
        pair = [bias_rows(2 * p), bias_rows(2 * p + 1)]
        dy, dx = place(7 * SUB, p % 2)
        for ref, c in ((keep, core), (send, 1 - core)):
            ref[dy, dx, p // 2, 64:72, :] = jnp.where(c == 0, pair[0], pair[1])
    for p in range(16):
        column = 128 * (p // 4)
        part = sums[:, column : column + 128].astype(bf16)
        dy, dx = place(7 * SUB, p % 2)
        keep[dy, dx, p // 2, 40:64, :] = part
        send[dy, dx, p // 2, 40:64, :] = part


def local_grads(pos, cot, left, right, ready):
    vmem = pltpu.VMEM
    scratch = [
        vmem((FRAMES + 32, D), f32),
        vmem((FRAMES + 16, D), f32),
        vmem((FRAMES + 16, D), f32),
        vmem((ROWS, D), f32),
        vmem((640 + 2 * LEFT, 128), f32),
        vmem((16, 1920), f32),
        vmem((PAIRS + 16, 1920), bf16),
        vmem((ROWS, D), f32),
        vmem((ROWS, 128), f32),
        vmem((ROWS, D), bf16),
        vmem((ROWS, FF), f32),
        vmem((ROWS, FF), f32),
        vmem((ROWS, FF), bf16),
        vmem((ROWS, D), f32),
        vmem((ROWS, D), bf16),
        vmem((ROWS, BINS), f32),
        vmem((ROWS, BINS), f32),
        vmem((ROWS, NFFT), bf16),
        vmem((ROWS, D), bf16),
        vmem((D, FF), f32),
        vmem((10, ROWS, 128), f32),
        vmem((ROWS, D), f32),
        vmem((24, D), f32),
        vmem((32, 128), f32),
        vmem((FF, D), f32),
        vmem((8, FF), f32),
    ]
    whole = pl.BlockSpec(memory_space=pltpu.VMEM)
    arrays = [cot, left, right, *ready]
    return pl.pallas_call(
        local_kernel,
        out_shape=(jax.ShapeDtypeStruct((4, 4, 8, SUB, 128), bf16),) * 2,
        in_specs=[pl.BlockSpec(memory_space=pltpu.SMEM)] + [whole] * len(arrays),
        out_specs=(whole, whole),
        scratch_shapes=scratch,
        compiler_params=pltpu.CompilerParams(vmem_limit_bytes=38 * 1024 * 1024),
        name="local_grads",
    )(pos, *arrays)


def unpack_kernel(t, up_g, head_g, down_g, embed_w, embed_b, depth_k, up_b, head_b, *vectors):
    f = lax.axis_index("frame")

    def tile(o):
        return t[o // SUB, o % SUB : o % SUB + 8, :].astype(f32)

    for columns, height, row, ref in ((12, 16, 0, up_g), (10, 16, 192, head_g), (4, 48, 352, down_g)):
        for j in range(columns):
            for h in range(height // 8):
                ref[h * 8 : h * 8 + 8, 128 * j : 128 * j + 128] = tile(row + j * height + h * 8)
    shift = 16 * (f % 8)
    back = lax.rem(128 - shift, 128)

    def rolled(x, by):
        return pltpu.roll(x, by, 1)

    embed_w[...] = rolled(tile(544), back)[:, 0:16]
    second = rolled(tile(552), back)
    third = rolled(tile(560), back)
    embed_b[...] = second[0:1, 0:16]
    depth_k[...] = second[1:8, 0:16]
    for i, ref in enumerate(vectors):
        ref[...] = third[i : i + 1, 0:16]
    last = tile(568)
    lane = lax.broadcasted_iota(jnp.int32, (1, 128), 1)
    for row, width, ref in ((0, 48, up_b), (2, 40, head_b)):
        shift = lax.rem(width * f, 128)
        back = lax.rem(128 - shift, 128)
        moved = rolled(last, back)
        joined = jnp.where(lane < 128 - shift, moved[row : row + 1, :], moved[row + 1 : row + 2, :])
        ref[...] = joined[:, 0:width]


def unpack(t):
    def shape(*s):
        return jax.ShapeDtypeStruct(s, f32)

    whole = pl.BlockSpec(memory_space=pltpu.VMEM)
    return pl.pallas_call(
        unpack_kernel,
        out_shape=(
            shape(16, FF), shape(16, NFFT), shape(48, D), shape(8, 16), shape(1, 16), shape(7, 16), shape(1, 48), shape(1, 40),
        ) + (shape(1, 16),) * 5,
        in_specs=[whole],
        out_specs=(whole,) * 13,
        name="unpack",
    )(t)


AXES = ("frame", "rec")


def index_of(z, yl, c, yh, x):
    return ((z * 2 + yl) * 2 + c) * 8 + yh * 4 + x


def groups_over(which):
    sizes = dict(z=8, yl=2, c=2, yh=2, x=4)
    kept = [n for n in sizes if n not in which]

    def walk(names, fixed):
        if not names:
            return [fixed]
        return [r for v in range(sizes[names[0]]) for r in walk(names[1:], {**fixed, names[0]: v})]

    return [[index_of(**g) for g in walk(list(which), fixed)] for fixed in walk(kept, {})]


def exchange(array, which):
    return lax.all_to_all(array, AXES, split_axis=0, concat_axis=0, axis_index_groups=groups_over(which), tiled=True)


def summed(array):
    return jnp.sum(array.astype(f32), axis=0)


def partners(which, offset=0):
    pairs = []
    for z in range(8):
        for y in range(4):
            for c in range(2):
                for x in range(4):
                    flip = 3 if offset else 1
                    to = dict(c=(y, 1 - c, x), x=(y, c, x ^ flip), y=(y ^ flip, c, x))[which]
                    pairs.append((index_of(z, y % 2, c, y // 2, x), index_of(z, to[0] % 2, to[1], to[0] // 2, to[2])))
    return pairs


ORDERS = ((0, 3, 1, 2), (0, 1, 3, 2))
AXIS_OF = ("x", "x", "y", "y")


def split_first(keep, other, *outs):
    for k in range(4):
        for i, d in enumerate(ORDERS[k % 2]):
            for e in range(4):
                for z in range(2):
                    at = ((e, d) if k < 2 else (d, e)) + (2 * k + z,)
                    total = keep[at].astype(f32) + other[at].astype(f32)
                    if i < 2:
                        outs[4 + k][i, e, z] = total
                    else:
                        outs[k][i - 2, e, z] = total.astype(bf16)


def split_second(*refs):
    keeps, others, outs = refs[0:4], refs[4:8], refs[8:]
    for k in range(4):
        for e in range(4):
            for z in range(2):
                outs[4 + k][e, z] = keeps[k][0, e, z] + others[k][0, e, z].astype(f32)
                outs[k][e, z] = (keeps[k][1, e, z] + others[k][1, e, z].astype(f32)).astype(bf16)


def split_third(*refs):
    keeps, others, outs = refs[0:4], refs[4:8], refs[8:]
    for g in range(2):
        for h in range(2):
            k = 2 * g + h
            for i, d in enumerate(ORDERS[0]):
                for z in range(2):
                    total = keeps[k][d, z] + others[k][d, z].astype(f32)
                    if i < 2:
                        outs[2 + g][i, 2 * h + z] = total
                    else:
                        outs[g][i - 2, 2 * h + z] = total.astype(bf16)


def split_fourth(*refs):
    keeps, others, outs = refs[0:2], refs[2:4], refs[4:]
    for g in range(2):
        for z in range(4):
            outs[2 + g][z] = keeps[g][0, z] + others[g][0, z].astype(f32)
            outs[g][z] = (keeps[g][1, z] + others[g][1, z].astype(f32)).astype(bf16)


def join(*refs):
    for g in range(2):
        for z in range(4):
            refs[4][4 * g + z] = (refs[g][z] + refs[2 + g][z].astype(f32)).astype(bf16)


def step(kernel, arrays, shape, count, limit):
    whole = pl.BlockSpec(memory_space=pltpu.VMEM)
    kinds = (bf16,) * count + (f32,) * (count if kernel is not join else 0)
    return pl.pallas_call(
        kernel,
        out_shape=tuple(jax.ShapeDtypeStruct(shape + (SUB, 128), kind) for kind in kinds),
        in_specs=[whole] * len(arrays),
        out_specs=(whole,) * len(kinds),
        compiler_params=pltpu.CompilerParams(vmem_limit_bytes=limit * 1024 * 1024),
        name=kernel.__name__,
    )(*arrays)


def reduce_all(keep, send):
    other = lax.ppermute(send, AXES, partners("c"))
    parts = step(split_first, (keep, other), (2, 4, 2), 4, 24)
    moved = [lax.ppermute(a, AXES, partners(AXIS_OF[k], k % 2)) for k, a in enumerate(parts[:4])]
    parts = step(split_second, (*parts[4:], *moved), (4, 2), 4, 16)
    moved = [lax.ppermute(a, AXES, partners(AXIS_OF[k], 1 - k % 2)) for k, a in enumerate(parts[:4])]
    parts = step(split_third, (*parts[4:], *moved), (2, 4), 2, 8)
    moved = [lax.ppermute(a, AXES, partners("yx"[g], 0)) for g, a in enumerate(parts[:2])]
    parts = step(split_fourth, (*parts[2:], *moved), (4,), 2, 8)
    moved = [lax.ppermute(a, AXES, partners("yx"[g], 1)) for g, a in enumerate(parts[:2])]
    (part,) = step(join, (*parts[2:], *moved), (8,), 1, 8)
    mine = summed(exchange(part, ("z",))).astype(bf16)
    return lax.all_to_all(jnp.broadcast_to(mine, (8, SUB, 128)), "rec", split_axis=0, concat_axis=0, tiled=True)


def body(code_indices, lengths, cotangent, *weights):
    count = lax.axis_size("frame")
    codes = code_indices[0].T
    samples = cotangent[0].astype(f32).reshape(640, 128)
    low = samples.astype(bf16)
    codes_low = codes.astype(bf16)
    forward = [(i, i + 1) for i in range(count - 1)]
    backward = [(b, a) for a, b in forward]
    left = lax.ppermute(jnp.concatenate([low[640 - LEFT :], codes_low[:, FRAMES - 128 :]]), "frame", forward)
    right = lax.ppermute(jnp.concatenate([low[:LEFT], codes_low[:, :128]]), "frame", backward)
    flat = [w if w.ndim == 2 else w[None] if w.size == D else w.reshape(-1, 128) for w in weights]
    ready = setup([codes, *flat, jnp.asarray(edges())])
    t = reduce_all(*local_grads(lengths, samples, left, right, ready))
    up_g, head_g, down_g, embed_w, embed_b, depth_k, up_b, head_b, *vectors = unpack(t)
    depth_b, gain, bias, down_b, scale = (v[0] for v in vectors)
    return (
        embed_w, embed_b[0], depth_k, depth_b, gain, bias, up_g, up_b[0], down_g, down_b, scale, head_g, head_b[0],
    )


def solution(mesh):
    return jax.shard_map(
        body,
        mesh=mesh,
        in_specs=(P("rec", "frame", None), P("rec"), P("rec", "frame")) + (P(),) * 13,
        out_specs=(
            P(None, "frame"), P("frame"), P(None, "frame"), P("frame"), P("frame"), P("frame"), P("frame", None),
            P("frame"), P("frame", None), P("frame"), P("frame"), P("frame", None), P("frame"),
        ),
        check_vma=False,
    )
```

```python
import jax
import jax.numpy as jnp
import numpy as np
from jax import lax
from jax.experimental import pallas as pl
from jax.experimental.pallas import tpu as pltpu
from jax.sharding import PartitionSpec as P

D = 512
FF = 1536
Q = 8
KERNEL = 7
NFFT = 1280
HOP = 320
BINS = 640
PAD = 480
EPSILON = 1e-06
HALF = 3.5

FRAMES = 256
PAIRS = FRAMES // 2
ROWS = FRAMES + 16
LEFT = 24
SUB = 72
TAB = 1472
f32 = jnp.float32
bf16 = jnp.bfloat16


def tables():
    n = np.arange(16)[:, None]
    k = np.arange(BINS)[None, :]
    turn = 2.0 * np.pi / NFFT
    out = np.zeros((64, BINS), np.float64)
    out[0:16] = np.cos(turn * (n * k % NFFT))
    out[16:32] = np.sin(turn * (n * k % NFFT))
    out[32] = np.cos(turn * (16 * k[0] % NFFT))
    out[33] = np.sin(turn * (16 * k[0] % NFFT))
    out[34] = np.where(k[0] == 0, 1.0, 2.0) / NFFT
    out[35] = np.where(k[0] == 0, 0.0, -2.0) / NFFT
    out[36] = np.cos(turn * 16)
    out[37] = np.sin(turn * 16)
    out[40:56, 0:128] = np.cos(turn * n)
    out[40:56, 128:256] = np.sin(turn * n)
    return out.astype(np.float32)


def edges():
    def square(i):
        return np.where((i >= 0) & (i < NFFT), (0.5 - 0.5 * np.cos(2.0 * np.pi / NFFT * i)) ** 2, 0.0)

    s = np.arange(512)
    first = sum(square(s + PAD - HOP * t) for t in range(4))
    last = sum(square(s - 32 + HOP * t) for t in range(1, 5))
    out = np.zeros((8, 128), np.float64)
    out[0:4] = (1.0 / first).reshape(4, 128)
    out[4:8] = (1.0 / last).reshape(4, 128)
    return out.astype(np.float32)


def dot(a, b):
    return lax.dot_general(a, b, (((1,), (0,)), ((), ())), preferred_element_type=f32)


def dot_rows(a, b):
    return lax.dot_general(a, b, (((0,), (0,)), ((), ())), preferred_element_type=f32)


def dot_cols(a, b):
    return lax.dot_general(a, b, (((1,), (1,)), ((), ())), preferred_element_type=f32)


def sine_cosine(p):
    k = jnp.round(p * np.float32(2.0 / np.pi))
    r = p - k * np.float32(1.5703125)
    r = r - k * np.float32(4.837512969970703125e-4)
    r = r - k * np.float32(7.54978995489188216e-8)
    z = r * r
    s = r + r * z * (np.float32(-1.6666654611e-1) + z * (np.float32(8.3321608736e-3) + z * np.float32(-1.9515295891e-4)))
    c = 1.0 - 0.5 * z + z * z * (
        np.float32(4.166664568298827e-2) + z * (np.float32(-1.388731625493765e-3) + z * np.float32(2.443315711809948e-5))
    )
    q = k.astype(jnp.int32)
    odd = (q & 1) == 1
    sine = jnp.where(odd, c, s)
    cosine = jnp.where(odd, s, c)
    sine = jnp.where((q & 2) == 2, -sine, sine)
    cosine = jnp.where(((q + 1) & 2) == 2, -cosine, cosine)
    return sine, cosine


def split3(w):
    hi = w.astype(bf16)
    rest = w - hi.astype(f32)
    mid = rest.astype(bf16)
    low = (rest - mid.astype(f32)).astype(bf16)
    return hi, mid, low


def setup_kernel(*refs):
    count = (len(refs) - 4) // 2
    sources, trig_far, outs = refs[:count], refs[count], refs[count + 1 : -3]
    tab, trig, sems = refs[-3:]
    first = pltpu.make_async_copy(trig_far, trig, sems.at[count])
    copies = [pltpu.make_async_copy(a, b, sems.at[i]) for i, (a, b) in enumerate(zip(sources, outs))]
    first.start()
    for copy in copies:
        copy.start()

    tab[0:96, :] = jnp.zeros((96, NFFT), bf16)
    tab[1376:TAB, :] = jnp.zeros((TAB - 1376, NFFT), bf16)
    first.wait()
    cs, sn = trig[32:33, :], trig[33:34, :]
    real_row, imag_row = trig[34:35, :], trig[35:36, :]
    wcs, wsn = trig[36:37, 0:128], trig[37:38, 0:128]

    def table_step(i, carry):
        c, s, wc, ws = carry
        window = jnp.concatenate([0.5 - 0.5 * wc] * 5, axis=1)
        at = pl.multiple_of(96 + i * 16, 16)
        tab[pl.ds(at, 16), 0:BINS] = (c * (window * real_row)).astype(bf16)
        tab[pl.ds(at, 16), BINS:] = (s * (window * imag_row)).astype(bf16)
        return c * cs - s * sn, s * cs + c * sn, wc * wcs - ws * wsn, ws * wcs + wc * wsn

    lax.fori_loop(0, NFFT // 16, table_step, (trig[0:16, :], trig[16:32, :], trig[40:56, 0:128], trig[40:56, 128:256]), unroll=4)
    for copy in copies:
        copy.wait()


def setup(arrays):
    whole = pl.BlockSpec(memory_space=pltpu.VMEM)
    return pl.pallas_call(
        setup_kernel,
        out_shape=tuple(jax.ShapeDtypeStruct(a.shape, a.dtype) for a in arrays) + (jax.ShapeDtypeStruct((TAB, NFFT), bf16),),
        in_specs=[pl.BlockSpec(memory_space=pltpu.HBM)] * (len(arrays) + 1),
        out_specs=(whole,) * (len(arrays) + 1),
        scratch_shapes=[pltpu.VMEM((64, BINS), f32), pltpu.SemaphoreType.DMA((len(arrays) + 1,))],
        compiler_params=pltpu.CompilerParams(vmem_limit_bytes=16 * 1024 * 1024),
        name="setup",
    )(*[pltpu.with_memory_space_constraint(a, pltpu.HBM) for a in (*arrays, jnp.asarray(tables()))])


def local_kernel(
    pos, cot, left, right, codes, embed_w, embed_b, depth_k, depth_b, gain, bias, up_w, up_b, down_w, down_b,
    scale, head_w, head_b, edge, tab, keep, send,
    feat, conv, cgrad, latg, samp, pair_rows, spec_in, xhat, rstd, normed, hid, dgelu, act, branch, latent, re, im,
    logit_low, low, big, spec, lg, sums, tiles, tall, rows,
):
    me, rec = lax.axis_index("frame"), lax.axis_index("rec")
    first_frame, length = me * FRAMES, pos[0]
    last_frame = lax.axis_size("frame") * FRAMES
    core, my, mx = me & 1, 2 * (rec >> 2) + ((me >> 1) & 1), rec & 3

    def place(o, yl):
        part = o // SUB
        return (2 * (part // 4) + yl) ^ my, (part % 4) ^ mx

    for t in range(FF // 128):
        rows[0:1, 128 * t : 128 * t + 128] = up_b[t : t + 1, :]
    for t in range(NFFT // 128):
        rows[1:2, 128 * t : 128 * t + 128] = head_b[t : t + 1, :]
    up_row, head_row = rows[0:1, :], rows[1:2, 0:NFFT]

    w_hi, w_mid, w_low = split3(embed_w[...])

    def project(c):
        c = c.astype(bf16)
        return (dot_rows(c, w_hi) + dot_rows(c, w_mid) + dot_rows(c, w_low)) * np.float32(1.0 / HALF) + embed_b[...]

    own_codes = codes[...].astype(f32) - HALF
    feat[0:16, :] = jnp.zeros((16, D), f32)
    feat[16 + FRAMES :, :] = jnp.zeros((feat.shape[0] - 16 - FRAMES, D), f32)
    feat[16 : 16 + FRAMES, :] = project(own_codes)
    feat[8:16, :] = project(left[LEFT:, :].astype(f32) - HALF)[120:128, :]
    feat[16 + FRAMES : 24 + FRAMES, :] = project(right[LEFT:, :].astype(f32) - HALF)[0:8, :]

    def mask_step(i, _):
        at = pl.multiple_of(8 + i * 8, 8)
        frame = first_frame + (at - 16) + lax.broadcasted_iota(jnp.int32, (8, D), 0)
        keep = (frame >= 0) & (frame < length)
        feat[pl.ds(at, 8), :] = jnp.where(keep, feat[pl.ds(at, 8), :], 0.0).astype(bf16).astype(f32)
        return 0

    lax.fori_loop(0, (FRAMES + 16) // 8, mask_step, 0, unroll=2)

    taps = [depth_k[j : j + 1, :] for j in range(KERNEL)]
    total = jnp.broadcast_to(depth_b[...], (FRAMES + 16, D))
    for j in range(KERNEL):
        total = total + taps[j] * feat[5 + j : 5 + j + FRAMES + 16, :]
    conv[...] = total

    def to_rows(ref, base, dst):
        dst[0:FRAMES, :] = ref[base : base + FRAMES, :]
        dst[FRAMES : FRAMES + 8, :] = ref[base - 8 : base, :]
        dst[FRAMES + 8 :, :] = ref[base + FRAMES : base + FRAMES + 8, :]

    to_rows(conv, 8, xhat)

    x = xhat[...]
    centre = x - jnp.mean(x, axis=1, keepdims=True)
    r = lax.rsqrt(jnp.mean(centre * centre, axis=1, keepdims=True) + EPSILON)
    x = centre * r
    xhat[...] = x
    rstd[...] = jnp.broadcast_to(r, (ROWS, 128))
    normed[...] = (x * gain[...] + bias[...]).astype(bf16)

    hid[...] = dot(normed[...], up_w[...])

    def gelu_step(i, _):
        at = pl.ds(pl.multiple_of(i * 16, 16), 16)
        x = hid[at, :] + up_row
        cdf = 0.5 + 0.5 * lax.erf(x * np.float32(0.7071067811865476))
        act[at, :] = (x * cdf).astype(bf16)
        dgelu[at, :] = cdf + x * (jnp.exp(-0.5 * x * x) * np.float32(0.3989422804014327))
        return 0

    lax.fori_loop(0, ROWS // 16, gelu_step, 0)

    branch[...] = dot(act[...], down_w[...]) + down_b[...]
    to_rows(feat, 16, lg)
    latent[...] = (lg[...] + scale[...] * branch[...]).astype(bf16)

    big[0:ROWS, 0:NFFT] = dot(latent[...], head_w[...])

    def head_step(i, _):
        at = pl.ds(pl.multiple_of(i * 16, 16), 16)
        magnitude = jnp.exp(big[at, 0:BINS] + head_row[:, 0:BINS])
        sine, cosine = sine_cosine(big[at, BINS:NFFT] + head_row[:, BINS:])
        re[at, :] = magnitude * cosine
        im[at, :] = magnitude * sine
        return 0

    lax.fori_loop(0, ROWS // 16, head_step, 0)

    samp[0:LEFT, :] = left[0:LEFT, :].astype(f32)
    samp[LEFT : LEFT + 640, :] = cot[...]
    samp[LEFT + 640 :, :] = right[0:LEFT, :].astype(f32)
    start = first_frame * HOP
    limit = length * HOP

    def sample_step(i, _):
        at = pl.multiple_of(i * 8, 8)
        row = at - LEFT + lax.broadcasted_iota(jnp.int32, (8, 128), 0)
        s = start + row * 128 + lax.broadcasted_iota(jnp.int32, (8, 128), 1)
        x = samp[pl.ds(at, 8), :] * np.float32(2.0 / 3.0)
        samp[pl.ds(at, 8), :] = jnp.where(s < limit, x, 0.0)
        return 0

    def fix(at, values):
        row = at - LEFT + lax.broadcasted_iota(jnp.int32, (4, 128), 0)
        s = start + row * 128 + lax.broadcasted_iota(jnp.int32, (4, 128), 1)
        samp[at : at + 4, :] = jnp.where(s < limit, cot[at - LEFT : at - LEFT + 4, :] * values, 0.0)

    lax.fori_loop(0, (LEFT * 2 + 640) // 8, sample_step, 0, unroll=2)

    @pl.when(first_frame == 0)
    def _():
        fix(LEFT, edge[0:4, :])

    @pl.when(first_frame + FRAMES == last_frame)
    def _():
        fix(LEFT + 636, edge[4:8, :])

    for d in range(3):
        for k in range(5):
            column = (d * 5 + k) * 128
            base = LEFT + (d - 1) * 5 + k
            spec_in[0:PAIRS, column : column + 128] = samp[pl.ds(base, PAIRS, stride=5), :].astype(bf16)
            pair_rows[0:2, column : column + 128] = samp[pl.ds(base - 10, 2, stride=5), :]
            pair_rows[2:4, column : column + 128] = samp[pl.ds(base + 640, 2, stride=5), :]
    pair_rows[4:16, :] = jnp.zeros((12, 1920), f32)
    spec_in[PAIRS : PAIRS + 16, :] = pair_rows[...].astype(bf16)

    even = dot(spec_in[:, 128:1536], tab[64:1472, :])
    odd = dot(spec_in[:, 384:1792], tab[0:1408, :])
    for t in range(10):
        column = slice(128 * t, 128 * t + 128)
        spec[t, FRAMES:, :] = jnp.zeros((16, 128), f32)
        for part, parity in ((even, 0), (odd, 1)):
            spec[t, pl.ds(parity, PAIRS, stride=2), :] = part[0:PAIRS, column]
            spec[t, pl.ds(FRAMES + 4 + parity, 4, stride=2), :] = part[PAIRS : PAIRS + 4, column]

    def logit_grad_of(at):
        das, dps = [], []
        for t in range(5):
            column = slice(128 * t, 128 * t + 128)
            g_re, g_im = spec[t, at, :], spec[t + 5, at, :]
            r, m = re[at, column], im[at, column]
            da = g_re * r + g_im * m
            dp = g_im * r - g_re * m
            logit_low[at, column] = da.astype(bf16)
            logit_low[at, BINS + 128 * t : BINS + 128 * t + 128] = dp.astype(bf16)
            das.append(da)
            dps.append(dp)
        return jnp.concatenate(das, axis=1), jnp.concatenate(dps, axis=1)

    def logit_step(i, carry):
        da, dp = logit_grad_of(pl.ds(pl.multiple_of(i * 16, 16), 16))
        return carry[0] + da[0:8] + da[8:16], carry[1] + dp[0:8] + dp[8:16]

    zero = jnp.zeros((8, BINS), f32)
    da, dp = lax.fori_loop(0, FRAMES // 16, logit_step, (zero, zero), unroll=2)
    logit_grad_of(pl.ds(FRAMES, 16))
    head_sum = jnp.concatenate([jnp.sum(da, axis=0, keepdims=True), jnp.sum(dp, axis=0, keepdims=True)], axis=1)
    for t in range(10):
        tiles[16 + t : 17 + t, :] = head_sum[:, 128 * t : 128 * t + 128]

    latg[...] = dot_cols(logit_low[...], head_w[...])

    def scatter(big_ref, columns, height, row):
        def step(p, _):
            z, yl = p // 2, p % 2
            for ref, f in ((keep, 2 * p + core), (send, 2 * p + 1 - core)):
                for j in range(columns):
                    for h in range(height // 8):
                        o = row + j * height + h * 8
                        at = pl.multiple_of(f * height + h * 8, 8)
                        value = big_ref[pl.ds(at, 8), 128 * j : 128 * j + 128].astype(bf16)
                        dy, dx = place(o, yl)
                        ref[dy, dx, z, o % SUB : o % SUB + 8, :] = value
            return 0

        lax.fori_loop(0, 16, step, 0)

    big[0:D, 0:NFFT] = dot_rows(latent[0:FRAMES, :], logit_low[0:FRAMES, :])
    scatter(big, 10, 16, 192)

    def latent_step(i, carry):
        at = pl.ds(pl.multiple_of(i * 16, 16), 16)
        g = latg[at, :]
        low[at, :] = (scale[...] * g).astype(bf16)
        b = g * branch[at, :]
        return carry[0] + b[0:8] + b[8:16], carry[1] + g[0:8] + g[8:16]

    zero = jnp.zeros((8, D), f32)
    scale_sum, latent_sum = lax.fori_loop(0, FRAMES // 16, latent_step, (zero, zero), unroll=2)
    low[FRAMES:, :] = (scale[...] * latg[FRAMES:, :]).astype(bf16)
    sums[20:21, :] = jnp.sum(scale_sum, axis=0, keepdims=True)
    sums[19:20, :] = jnp.sum(latent_sum, axis=0, keepdims=True) * scale[...]

    tall[...] = dot_rows(act[0:FRAMES, :], low[0:FRAMES, :])
    scatter(tall, 4, 48, 352)

    hid[...] = dot_cols(low[...], down_w[...])

    def hidden_grad_of(at):
        g = hid[at, :] * dgelu[at, :]
        act[at, :] = g.astype(bf16)
        return g

    def hidden_step(i, carry):
        g = hidden_grad_of(pl.ds(pl.multiple_of(i * 16, 16), 16))
        return carry + g[0:8] + g[8:16]

    up_sum = lax.fori_loop(0, FRAMES // 16, hidden_step, jnp.zeros((8, FF), f32), unroll=2)
    hidden_grad_of(pl.ds(FRAMES, 16))
    up_sum = jnp.sum(up_sum, axis=0, keepdims=True)
    for t in range(12):
        tiles[t : t + 1, :] = up_sum[:, 128 * t : 128 * t + 128]

    big[0:D, 0:FF] = dot_rows(normed[0:FRAMES, :], act[0:FRAMES, :])
    scatter(big, 12, 16, 0)

    lg[...] = dot_cols(act[...], up_w[...])

    g, x = lg[...], xhat[...]
    dx = g * gain[...]
    m1 = jnp.mean(dx, axis=1, keepdims=True)
    m2 = jnp.mean(dx * x, axis=1, keepdims=True)
    lg[...] = rstd[:, 0:1] * (dx - m1 - x * m2)
    sums[17:18, :] = jnp.sum(g[0:FRAMES] * x[0:FRAMES], axis=0, keepdims=True)
    sums[18:19, :] = jnp.sum(g[0:FRAMES], axis=0, keepdims=True)

    i = lax.broadcasted_iota(jnp.int32, (16, D), 0)
    frame = jnp.where(i < 8, i - 8, i + (FRAMES - 8)) + first_frame
    inside = (frame >= 0) & (frame < last_frame)
    edge_rows = jnp.where(inside, lg[FRAMES:, :], 0.0)

    cgrad[0:8, :] = edge_rows[0:8]
    cgrad[8 : 8 + FRAMES, :] = lg[0:FRAMES, :]
    cgrad[8 + FRAMES :, :] = edge_rows[8:16]

    own = cgrad[8 : 8 + FRAMES, :]
    sums[16:17, :] = jnp.sum(own, axis=0, keepdims=True)
    total = latg[0:FRAMES, :]
    for j in range(KERNEL):
        sums[9 + j : 10 + j, :] = jnp.sum(own * feat[13 + j : 13 + j + FRAMES, :], axis=0, keepdims=True)
        total = total + taps[j] * cgrad[11 - j : 11 - j + FRAMES, :]
    frame = first_frame + lax.broadcasted_iota(jnp.int32, (FRAMES, D), 0)
    total = jnp.where(frame < length, total, 0.0)
    sums[8:9, :] = jnp.sum(total, axis=0, keepdims=True)
    hi, mid, rest = split3(total)
    own_low = own_codes.astype(bf16)
    sums[0:8, :] = (dot(own_low, hi) + dot(own_low, mid) + dot(own_low, rest)) * np.float32(1.0 / HALF)
    sums[21:24, :] = jnp.zeros((3, D), f32)

    tiles[12:16, :] = jnp.zeros((4, 128), f32)
    tiles[26:32, :] = jnp.zeros((6, 128), f32)
    blank = jnp.zeros((4, 128), f32)

    def bias_rows(f):
        up, head = 48 * f // 128, 16 + 40 * f // 128
        return jnp.concatenate([tiles[up : up + 2, :], tiles[head : head + 2, :], blank], axis=0).astype(bf16)

    for p in range(16):
        pair = [bias_rows(2 * p), bias_rows(2 * p + 1)]
        dy, dx = place(7 * SUB, p % 2)
        for ref, c in ((keep, core), (send, 1 - core)):
            ref[dy, dx, p // 2, 64:72, :] = jnp.where(c == 0, pair[0], pair[1])
    for p in range(16):
        column = 128 * (p // 4)
        part = sums[:, column : column + 128].astype(bf16)
        dy, dx = place(7 * SUB, p % 2)
        keep[dy, dx, p // 2, 40:64, :] = part
        send[dy, dx, p // 2, 40:64, :] = part


def local_grads(pos, cot, left, right, ready):
    vmem = pltpu.VMEM
    scratch = [
        vmem((FRAMES + 32, D), f32),
        vmem((FRAMES + 16, D), f32),
        vmem((FRAMES + 16, D), f32),
        vmem((ROWS, D), f32),
        vmem((640 + 2 * LEFT, 128), f32),
        vmem((16, 1920), f32),
        vmem((PAIRS + 16, 1920), bf16),
        vmem((ROWS, D), f32),
        vmem((ROWS, 128), f32),
        vmem((ROWS, D), bf16),
        vmem((ROWS, FF), f32),
        vmem((ROWS, FF), f32),
        vmem((ROWS, FF), bf16),
        vmem((ROWS, D), f32),
        vmem((ROWS, D), bf16),
        vmem((ROWS, BINS), f32),
        vmem((ROWS, BINS), f32),
        vmem((ROWS, NFFT), bf16),
        vmem((ROWS, D), bf16),
        vmem((D, FF), f32),
        vmem((10, ROWS, 128), f32),
        vmem((ROWS, D), f32),
        vmem((24, D), f32),
        vmem((32, 128), f32),
        vmem((FF, D), f32),
        vmem((8, FF), f32),
    ]
    whole = pl.BlockSpec(memory_space=pltpu.VMEM)
    arrays = [cot, left, right, *ready]
    return pl.pallas_call(
        local_kernel,
        out_shape=(jax.ShapeDtypeStruct((4, 4, 8, SUB, 128), bf16),) * 2,
        in_specs=[pl.BlockSpec(memory_space=pltpu.SMEM)] + [whole] * len(arrays),
        out_specs=(whole, whole),
        scratch_shapes=scratch,
        compiler_params=pltpu.CompilerParams(vmem_limit_bytes=38 * 1024 * 1024),
        name="local_grads",
    )(pos, *arrays)


def unpack_kernel(t, up_g, head_g, down_g, embed_w, embed_b, depth_k, up_b, head_b, *vectors):
    f = lax.axis_index("frame")

    def tile(o):
        return t[o // SUB, o % SUB : o % SUB + 8, :].astype(f32)

    for columns, height, row, ref in ((12, 16, 0, up_g), (10, 16, 192, head_g), (4, 48, 352, down_g)):
        for j in range(columns):
            for h in range(height // 8):
                ref[h * 8 : h * 8 + 8, 128 * j : 128 * j + 128] = tile(row + j * height + h * 8)
    shift = 16 * (f % 8)
    back = lax.rem(128 - shift, 128)

    def rolled(x, by):
        return pltpu.roll(x, by, 1)

    embed_w[...] = rolled(tile(544), back)[:, 0:16]
    second = rolled(tile(552), back)
    third = rolled(tile(560), back)
    embed_b[...] = second[0:1, 0:16]
    depth_k[...] = second[1:8, 0:16]
    for i, ref in enumerate(vectors):
        ref[...] = third[i : i + 1, 0:16]
    last = tile(568)
    lane = lax.broadcasted_iota(jnp.int32, (1, 128), 1)
    for row, width, ref in ((0, 48, up_b), (2, 40, head_b)):
        shift = lax.rem(width * f, 128)
        back = lax.rem(128 - shift, 128)
        moved = rolled(last, back)
        joined = jnp.where(lane < 128 - shift, moved[row : row + 1, :], moved[row + 1 : row + 2, :])
        ref[...] = joined[:, 0:width]


def unpack(t):
    def shape(*s):
        return jax.ShapeDtypeStruct(s, f32)

    whole = pl.BlockSpec(memory_space=pltpu.VMEM)
    return pl.pallas_call(
        unpack_kernel,
        out_shape=(
            shape(16, FF), shape(16, NFFT), shape(48, D), shape(8, 16), shape(1, 16), shape(7, 16), shape(1, 48), shape(1, 40),
        ) + (shape(1, 16),) * 5,
        in_specs=[whole],
        out_specs=(whole,) * 13,
        name="unpack",
    )(t)


AXES = ("frame", "rec")


def index_of(z, yl, c, yh, x):
    return ((z * 2 + yl) * 2 + c) * 8 + yh * 4 + x


def groups_over(which):
    sizes = dict(z=8, yl=2, c=2, yh=2, x=4)
    kept = [n for n in sizes if n not in which]

    def walk(names, fixed):
        if not names:
            return [fixed]
        return [r for v in range(sizes[names[0]]) for r in walk(names[1:], {**fixed, names[0]: v})]

    return [[index_of(**g) for g in walk(list(which), fixed)] for fixed in walk(kept, {})]


def exchange(array, which):
    return lax.all_to_all(array, AXES, split_axis=0, concat_axis=0, axis_index_groups=groups_over(which), tiled=True)


def summed(array):
    return jnp.sum(array.astype(f32), axis=0)


def partners(which, offset=0):
    pairs = []
    for z in range(8):
        for y in range(4):
            for c in range(2):
                for x in range(4):
                    flip = 3 if offset else 1
                    to = dict(c=(y, 1 - c, x), x=(y, c, x ^ flip), y=(y ^ flip, c, x))[which]
                    pairs.append((index_of(z, y % 2, c, y // 2, x), index_of(z, to[0] % 2, to[1], to[0] // 2, to[2])))
    return pairs


ORDERS = ((0, 3, 1, 2), (0, 1, 3, 2))
AXIS_OF = ("x", "x", "y", "y")


def split_first(keep, other, *outs):
    for k in range(4):
        for i, d in enumerate(ORDERS[k % 2]):
            for e in range(4):
                for z in range(2):
                    at = ((e, d) if k < 2 else (d, e)) + (2 * k + z,)
                    total = keep[at].astype(f32) + other[at].astype(f32)
                    if i < 2:
                        outs[4 + k][i, e, z] = total
                    else:
                        outs[k][i - 2, e, z] = total.astype(bf16)


def split_second(*refs):
    keeps, others, outs = refs[0:4], refs[4:8], refs[8:]
    for k in range(4):
        for e in range(4):
            for z in range(2):
                outs[4 + k][e, z] = keeps[k][0, e, z] + others[k][0, e, z].astype(f32)
                outs[k][e, z] = (keeps[k][1, e, z] + others[k][1, e, z].astype(f32)).astype(bf16)


def split_third(*refs):
    keeps, others, outs = refs[0:4], refs[4:8], refs[8:]
    for g in range(2):
        for h in range(2):
            k = 2 * g + h
            for i, d in enumerate(ORDERS[0]):
                for z in range(2):
                    total = keeps[k][d, z] + others[k][d, z].astype(f32)
                    if i < 2:
                        outs[2 + g][i, 2 * h + z] = total
                    else:
                        outs[g][i - 2, 2 * h + z] = total.astype(bf16)


def split_fourth(*refs):
    keeps, others, outs = refs[0:2], refs[2:4], refs[4:]
    for g in range(2):
        for z in range(4):
            outs[2 + g][z] = keeps[g][0, z] + others[g][0, z].astype(f32)
            outs[g][z] = (keeps[g][1, z] + others[g][1, z].astype(f32)).astype(bf16)


def join(*refs):
    for g in range(2):
        for z in range(4):
            refs[4][4 * g + z] = (refs[g][z] + refs[2 + g][z].astype(f32)).astype(bf16)


def step(kernel, arrays, shape, count, limit):
    whole = pl.BlockSpec(memory_space=pltpu.VMEM)
    kinds = (bf16,) * count + (f32,) * (count if kernel is not join else 0)
    return pl.pallas_call(
        kernel,
        out_shape=tuple(jax.ShapeDtypeStruct(shape + (SUB, 128), kind) for kind in kinds),
        in_specs=[whole] * len(arrays),
        out_specs=(whole,) * len(kinds),
        compiler_params=pltpu.CompilerParams(vmem_limit_bytes=limit * 1024 * 1024),
        name=kernel.__name__,
    )(*arrays)


def reduce_all(keep, send):
    other = lax.ppermute(send, AXES, partners("c"))
    parts = step(split_first, (keep, other), (2, 4, 2), 4, 24)
    moved = [lax.ppermute(a, AXES, partners(AXIS_OF[k], k % 2)) for k, a in enumerate(parts[:4])]
    parts = step(split_second, (*parts[4:], *moved), (4, 2), 4, 16)
    moved = [lax.ppermute(a, AXES, partners(AXIS_OF[k], 1 - k % 2)) for k, a in enumerate(parts[:4])]
    parts = step(split_third, (*parts[4:], *moved), (2, 4), 2, 8)
    moved = [lax.ppermute(a, AXES, partners("yx"[g], 0)) for g, a in enumerate(parts[:2])]
    parts = step(split_fourth, (*parts[2:], *moved), (4,), 2, 8)
    moved = [lax.ppermute(a, AXES, partners("yx"[g], 1)) for g, a in enumerate(parts[:2])]
    (part,) = step(join, (*parts[2:], *moved), (8,), 1, 8)
    mine = summed(exchange(part, ("z",))).astype(bf16)
    return lax.all_to_all(jnp.broadcast_to(mine, (8, SUB, 128)), "rec", split_axis=0, concat_axis=0, tiled=True)


def body(code_indices, lengths, cotangent, *weights):
    count = lax.axis_size("frame")
    codes = code_indices[0].T
    samples = cotangent[0].astype(f32).reshape(640, 128)
    low = samples.astype(bf16)
    codes_low = codes.astype(bf16)
    forward = [(i, i + 1) for i in range(count - 1)]
    backward = [(b, a) for a, b in forward]
    left = lax.ppermute(jnp.concatenate([low[640 - LEFT :], codes_low[:, FRAMES - 128 :]]), "frame", forward)
    right = lax.ppermute(jnp.concatenate([low[:LEFT], codes_low[:, :128]]), "frame", backward)
    flat = [w if w.ndim == 2 else w[None] if w.size == D else w.reshape(-1, 128) for w in weights]
    ready = setup([codes, *flat, jnp.asarray(edges())])
    t = reduce_all(*local_grads(lengths, samples, left, right, ready))
    up_g, head_g, down_g, embed_w, embed_b, depth_k, up_b, head_b, *vectors = unpack(t)
    depth_b, gain, bias, down_b, scale = (v[0] for v in vectors)
    return (
        embed_w, embed_b[0], depth_k, depth_b, gain, bias, up_g, up_b[0], down_g, down_b, scale, head_g, head_b[0],
    )


def solution(mesh):
    return jax.shard_map(
        body,
        mesh=mesh,
        in_specs=(P("rec", "frame", None), P("rec"), P("rec", "frame")) + (P(),) * 13,
        out_specs=(
            P(None, "frame"), P("frame"), P(None, "frame"), P("frame"), P("frame"), P("frame"), P("frame", None),
            P("frame"), P("frame", None), P("frame"), P("frame"), P("frame", None), P("frame"),
        ),
        check_vma=False,
    )
```
